32 devices in a mesh: data: 2 (over x), pp: 4 (over z), ep: 4 (over y, core).
Axes of the slice: x: 2, y: 2, z: 4, core: 2. Of those that a mesh axis runs over, the one named last changes fastest.
Arguments:
- expert_out: bfloat16 [4, 2, 256, 32, 4096], P('pp', 'data', 'ep'), parts along dimension 1
- expert_ids: int32 [4, 2, 12, 64, 8], P('pp', 'data', 'ep'), parts along dimension 1
- slot_ids: int32 [4, 2, 12, 64, 8], P('pp', 'data', 'ep'), parts along dimension 1
- gate_weights: float32 [4, 2, 12, 64, 8], P('pp', 'data', 'ep'), parts along dimension 1
- residual: bfloat16 [4, 2, 12, 64, 4096], P('pp', 'data', 'ep'), parts along dimension 1
- norm_moe: float32 [4, 4096], P('pp')
- w_gate: bfloat16 [4, 4096, 1024], P('pp')
- w_up: bfloat16 [4, 4096, 1024], P('pp')
- w_down: bfloat16 [4, 1024, 4096], P('pp')
- norm_attn: float32 [4, 4096], P('pp')
- w_query: bfloat16 [4, 4096, 32, 128], P('pp')
- w_key: bfloat16 [4, 4096, 32, 128], P('pp')
- w_value: bfloat16 [4, 4096, 32, 128], P('pp')
- w_out: bfloat16 [4, 32, 128, 4096], P('pp')
Outputs:
- output: bfloat16 [4, 2, 12, 64, 4096], P('pp', 'data', 'ep'), parts along dimension 1
There are 2 independent parts. The reference program is written for one: setup_inputs(seed, part) draws one part's arguments, and reference() takes and returns one part's arrays. A program takes and returns all parts, laid end to end along the dimension named above; an argument that names none is the same for every part.
All inputs are finite; a program needn't handle non-finite values.
Results may differ from the reference program's by a relative error of at most 0.0155369.
Values are sent between devices in bfloat16 or wider.
A program may use at most 1 GiB of HBM per device.

```python
import math
import jax
import jax.numpy as jnp
from jax import lax

STAGES = 4
EP_SIZE = 4
MICRO_BATCHES = 1
SEQ_DEV = 3
SEQ_LEN = 64
D_MODEL = 4096
NUM_HEADS = 32
HEAD_DIM = 128
EXPERTS = 256
TOP_K = 8
FF_SHARED = 1024
CAP_SLOTS = 8

SEQS = EP_SIZE * SEQ_DEV
TOK_DEV = SEQ_DEV * SEQ_LEN
TOKENS = SEQS * SEQ_LEN
SLOTS = EP_SIZE * CAP_SLOTS
HEADS_WIDTH = NUM_HEADS * HEAD_DIM
SCORE_SCALE = 1.0 / math.sqrt(HEAD_DIM)
EPSILON = 1e-6


def route_group(group_args):
    group_key, hot_draw = group_args
    hot_rank = jnp.argsort(jnp.argsort(hot_draw * EXPERTS + jnp.arange(EXPERTS)))
    lead_mask = (jnp.arange(TOK_DEV) <= CAP_SLOTS).astype(jnp.int32)[:, None]
    hot_bias = jnp.where(hot_rank < max(1, TOP_K // 4), 1024, 0) + jnp.where(hot_rank == 0, 8192, 0) * lead_mask
    noise_draw = jax.random.randint(group_key, (EP_SIZE, TOK_DEV, EXPERTS), 0, 4096)
    scores = (noise_draw + hot_bias) * EXPERTS + jnp.arange(EXPERTS)
    top_vals, expert_ids = lax.top_k(scores, TOP_K)
    choice_count = TOK_DEV * TOP_K
    flat_ids = expert_ids.reshape(EP_SIZE, choice_count)
    position = jnp.arange(choice_count)
    sort_order = jnp.argsort(flat_ids * choice_count + position, axis=-1)
    sorted_ids = jnp.take_along_axis(flat_ids, sort_order, axis=-1)
    is_start = jnp.concatenate([jnp.ones((EP_SIZE, 1), jnp.bool_), sorted_ids[:, 1:] != sorted_ids[:, :-1]], axis=1)
    start_pos = lax.cummax(jnp.where(is_start, position, 0), axis=1)
    slot_rank = jnp.take_along_axis(position - start_pos, jnp.argsort(sort_order, axis=-1), axis=-1)
    source = jnp.arange(EP_SIZE)[:, None]
    slot_ids = jnp.where(slot_rank < CAP_SLOTS, source * CAP_SLOTS + slot_rank, -1)
    return expert_ids.reshape(SEQS, SEQ_LEN, TOP_K), slot_ids.reshape(SEQS, SEQ_LEN, TOP_K)


def draw_routing(key):
    key_hot, key_score = jax.random.split(key)
    hot_draw = jax.random.randint(key_hot, (STAGES * MICRO_BATCHES, EXPERTS), 0, 1 << 20)
    group_keys = jax.random.split(key_score, STAGES * MICRO_BATCHES)
    expert_ids, slot_ids = lax.map(route_group, (group_keys, hot_draw))
    route_shape = (STAGES, MICRO_BATCHES, SEQS, SEQ_LEN, TOP_K)
    return expert_ids.reshape(route_shape), slot_ids.reshape(route_shape)


def setup_inputs(seed: int = 0, part: int = 0) -> dict:
    base_key = jax.random.key(seed)
    part_keys = jax.random.split(jax.random.fold_in(base_key, part), 5)
    expert_ids, slot_ids = draw_routing(part_keys[0])
    route_shape = (STAGES, MICRO_BATCHES, SEQS, SEQ_LEN, TOP_K)
    gate_draw = jax.random.normal(part_keys[1], route_shape, jnp.float32)
    gate_weights = jnp.exp(1.2 * gate_draw - 0.72) / TOP_K
    expert_scale = jax.random.uniform(part_keys[2], (STAGES * MICRO_BATCHES, EXPERTS, 1, 1), jnp.float32, 0.5, 3.0)
    out_keys = jax.random.split(part_keys[3], STAGES * MICRO_BATCHES)

    def draw_outputs(group_args):
        group_key, group_scale = group_args
        normal_draw = jax.random.normal(group_key, (EXPERTS, SLOTS, D_MODEL), jnp.float32)
        return (normal_draw * group_scale).astype(jnp.bfloat16)

    expert_out = lax.map(draw_outputs, (out_keys, expert_scale)).reshape(STAGES, MICRO_BATCHES, EXPERTS, SLOTS, D_MODEL)
    residual = jax.random.normal(part_keys[4], (STAGES, MICRO_BATCHES, SEQS, SEQ_LEN, D_MODEL), jnp.float32).astype(jnp.bfloat16)
    weight_keys = jax.random.split(jax.random.key(seed + 1), 9)
    in_scale = 1.0 / math.sqrt(D_MODEL)
    down_scale = 2.0 / math.sqrt(FF_SHARED)
    query_scale = 1.5 / math.sqrt(D_MODEL)
    out_scale = math.sqrt(math.sqrt(SEQ_LEN)) / math.sqrt(HEADS_WIDTH)
    norm_moe = jax.random.uniform(weight_keys[0], (STAGES, D_MODEL), jnp.float32, 0.5, 1.5)
    w_gate = (jax.random.normal(weight_keys[1], (STAGES, D_MODEL, FF_SHARED), jnp.float32) * in_scale).astype(jnp.bfloat16)
    w_up = (jax.random.normal(weight_keys[2], (STAGES, D_MODEL, FF_SHARED), jnp.float32) * in_scale).astype(jnp.bfloat16)
    w_down = (jax.random.normal(weight_keys[3], (STAGES, FF_SHARED, D_MODEL), jnp.float32) * down_scale).astype(jnp.bfloat16)
    norm_attn = jax.random.uniform(weight_keys[4], (STAGES, D_MODEL), jnp.float32, 0.5, 1.5)
    w_query = (jax.random.normal(weight_keys[5], (STAGES, D_MODEL, NUM_HEADS, HEAD_DIM), jnp.float32) * query_scale).astype(jnp.bfloat16)
    w_key = (jax.random.normal(weight_keys[6], (STAGES, D_MODEL, NUM_HEADS, HEAD_DIM), jnp.float32) * in_scale).astype(jnp.bfloat16)
    w_value = (jax.random.normal(weight_keys[7], (STAGES, D_MODEL, NUM_HEADS, HEAD_DIM), jnp.float32) * in_scale).astype(jnp.bfloat16)
    w_out = (jax.random.normal(weight_keys[8], (STAGES, NUM_HEADS, HEAD_DIM, D_MODEL), jnp.float32) * out_scale).astype(jnp.bfloat16)
    return {"expert_out": expert_out, "expert_ids": expert_ids, "slot_ids": slot_ids, "gate_weights": gate_weights, "residual": residual, "norm_moe": norm_moe, "w_gate": w_gate, "w_up": w_up, "w_down": w_down, "norm_attn": norm_attn, "w_query": w_query, "w_key": w_key, "w_value": w_value, "w_out": w_out}


def rms_norm(tensor, gain):
    values = tensor.astype(jnp.float32)
    inv_rms = lax.rsqrt(jnp.mean(values * values, axis=-1, keepdims=True) + EPSILON)
    return values * inv_rms * gain


def shared_expert(residual, norm_moe, w_gate, w_up, w_down):
    normed = rms_norm(residual, norm_moe).astype(jnp.bfloat16)
    gate_act = jnp.dot(normed, w_gate, preferred_element_type=jnp.float32)
    up_act = jnp.dot(normed, w_up, preferred_element_type=jnp.float32)
    hidden = (jax.nn.silu(gate_act) * up_act).astype(jnp.bfloat16)
    return jnp.dot(hidden, w_down, preferred_element_type=jnp.float32).astype(jnp.bfloat16)


def combine_micro(micro_args, stage_weights):
    expert_out, expert_ids, slot_ids, gate_weights, residual = micro_args
    norm_moe, w_gate, w_up, w_down = stage_weights
    flat_slots = slot_ids.reshape(TOKENS, TOP_K)
    kept_mask = flat_slots >= 0
    row_ids = expert_ids.reshape(TOKENS, TOP_K) * SLOTS + jnp.where(kept_mask, flat_slots, 0)
    picked = jnp.take(expert_out.reshape(EXPERTS * SLOTS, D_MODEL), row_ids, axis=0)
    weights = jnp.where(kept_mask, gate_weights.reshape(TOKENS, TOP_K), 0.0)
    routed = jnp.sum(picked.astype(jnp.float32) * weights[:, :, None], axis=1)
    flat_resid = residual.reshape(TOKENS, D_MODEL)
    shared = shared_expert(flat_resid, norm_moe, w_gate, w_up, w_down)
    combined = flat_resid.astype(jnp.float32) + shared.astype(jnp.float32) + routed
    return combined.astype(jnp.bfloat16).reshape(SEQS, SEQ_LEN, D_MODEL)


def attend_sequence(seq_args):
    queries, key_heads, value_heads = seq_args
    scores = jnp.einsum("qhe,khe->hqk", queries.astype(jnp.float32), key_heads.astype(jnp.float32)) * SCORE_SCALE
    causal = jnp.arange(SEQ_LEN)[:, None] >= jnp.arange(SEQ_LEN)[None, :]
    scores = jnp.where(causal, scores, -1e30)
    attn_probs = jnp.exp(scores - jnp.max(scores, axis=-1, keepdims=True))
    prob_sum = jnp.sum(attn_probs, axis=-1, keepdims=True)
    attn_mixed = jnp.einsum("hqk,khe->hqe", attn_probs.astype(jnp.bfloat16).astype(jnp.float32), value_heads.astype(jnp.float32))
    return attn_mixed / prob_sum


def attention_stage(stage_args):
    received, norm_attn, w_query, w_key, w_value, w_out = stage_args
    seq_count = MICRO_BATCHES * SEQS
    normed = rms_norm(received, norm_attn).astype(jnp.bfloat16).reshape(seq_count * SEQ_LEN, D_MODEL)

    def project(weight):
        product = jnp.dot(normed, weight.reshape(D_MODEL, HEADS_WIDTH), preferred_element_type=jnp.float32)
        return product.astype(jnp.bfloat16).reshape(seq_count, SEQ_LEN, NUM_HEADS, HEAD_DIM)

    attn_mixed = lax.map(attend_sequence, (project(w_query), project(w_key), project(w_value)))
    mixed_rows = jnp.transpose(attn_mixed.astype(jnp.bfloat16), (0, 2, 1, 3)).reshape(seq_count * SEQ_LEN, HEADS_WIDTH)
    attn_proj = jnp.dot(mixed_rows, w_out.reshape(HEADS_WIDTH, D_MODEL), preferred_element_type=jnp.float32).astype(jnp.bfloat16)
    updated = received.astype(jnp.float32) + attn_proj.astype(jnp.float32).reshape(received.shape)
    return updated.astype(jnp.bfloat16)


def reference(expert_out, expert_ids, slot_ids, gate_weights, residual, norm_moe, w_gate, w_up, w_down, norm_attn, w_query, w_key, w_value, w_out):
    def combine_stage(stage_args):
        def one_micro(micro_args):
            return combine_micro(micro_args, stage_args[5:])
        return lax.map(one_micro, stage_args[:5])

    combined = lax.map(combine_stage, (expert_out, expert_ids, slot_ids, gate_weights, residual, norm_moe, w_gate, w_up, w_down))
    received = jnp.roll(combined, 1, axis=0)
    return lax.map(attention_stage, (received, norm_attn, w_query, w_key, w_value, w_out))
```

```python
import math
import functools
import jax
import jax.numpy as jnp
from jax import lax
from jax.experimental import pallas as pl
from jax.experimental.pallas import tpu as pltpu
from jax.sharding import PartitionSpec as P

EPSILON = 1e-6
MESH = pl.DeviceIdType.MESH
CHUNK = 32
COLS = 512


def rms_norm(tensor, gain):
    values = tensor.astype(jnp.float32)
    inv_rms = lax.rsqrt(jnp.mean(values * values, axis=-1, keepdims=True) + EPSILON)
    return values * inv_rms * gain


def combine_kernel(
    meta_ref, expert_ref, resid_hbm, norm_ref, gate_hbm, up_hbm, down_hbm, out_ref,
    tab, meta_in, meta_t, pieces, diag_out, diag_in, cross, part_out, part_in, arrive, base,
    resid, normed, hidden, y_out, w_gate, w_up, w_down,
    tab_sem, meta_send, meta_recv, diag_send, diag_recv, part_send, part_recv,
    cross_send, cross_recv, y_send, y_recv, resid_sem, gate_sem, up_sem, down_sem,
):
    tokens, dim = resid.shape
    chunks = tokens // CHUNK
    rows_owner = tab.shape[1] * tab.shape[2]
    slots = tab.shape[2]
    ff_dim = hidden.shape[1]
    me = lax.axis_index("ep")
    stage = lax.axis_index("pp")
    y_pos, core = me // 2, me % 2
    pair = y_pos * 2 + (1 - core)
    across = (1 - y_pos) * 2 + core
    diagonal = (1 - y_pos) * 2 + (1 - core)
    next_stage, prev_stage = (stage + 1) % 4, (stage + 3) % 4

    owners = (diagonal, across, pair, me)

    def table_copy(k):
        start = pl.multiple_of(owners[k] * slots, slots)
        return pltpu.make_async_copy(expert_ref.at[:, pl.ds(start, slots), :], tab.at[k], tab_sem.at[k])

    def resid_copy():
        return pltpu.make_async_copy(resid_hbm, resid, resid_sem)

    ff_tile = w_gate.shape[2]

    def gate_copy(n, slot):
        cols = pl.ds(pl.multiple_of(n * ff_tile, ff_tile), ff_tile)
        return pltpu.make_async_copy(gate_hbm.at[:, cols], w_gate.at[slot], gate_sem.at[slot])

    def up_copy(n, slot):
        cols = pl.ds(pl.multiple_of(n * ff_tile, ff_tile), ff_tile)
        return pltpu.make_async_copy(up_hbm.at[:, cols], w_up.at[slot], up_sem.at[slot])

    def down_copy(n, slot):
        cols = pl.ds(pl.multiple_of(n * COLS, COLS), COLS)
        return pltpu.make_async_copy(down_hbm.at[:, cols], w_down.at[slot], down_sem.at[slot])

    for k in range(4):
        table_copy(k).start()
    resid_copy().start()
    for slot in range(2):
        gate_copy(slot, slot).start()
        up_copy(slot, slot).start()
        down_copy(slot, slot).start()

    barrier = pltpu.get_barrier_semaphore()
    for peer in (pair, across, diagonal):
        pl.semaphore_signal(barrier, inc=1, device_id={"ep": peer}, device_id_type=MESH)
    for peer in (next_stage, prev_stage):
        pl.semaphore_signal(barrier, inc=1, device_id={"pp": peer}, device_id_type=MESH)
    pl.semaphore_wait(barrier, 5)

    def meta_copy(k):
        return pltpu.make_async_remote_copy(
            src_ref=meta_ref, dst_ref=meta_in.at[k], send_sem=meta_send.at[k], recv_sem=meta_recv.at[k],
            device_id={"ep": owners[k]}, device_id_type=MESH)

    for k in range(3):
        meta_copy(k).start()

    def rows_of(c):
        return pl.ds(pl.multiple_of(c * CHUNK, CHUNK), CHUNK)

    def row_copy(src, dst, send, recv, target, c):
        return pltpu.make_async_remote_copy(
            src_ref=src.at[rows_of(c), :], dst_ref=dst.at[rows_of(c), :], send_sem=send.at[c], recv_sem=recv.at[c],
            device_id=target, device_id_type=MESH)

    def diag_copy(c):
        return row_copy(diag_out, diag_in, diag_send, diag_recv, {"ep": pair}, c)

    def part_copy(c):
        return row_copy(part_out, part_in, part_send, part_recv, {"ep": pair}, c)

    def cross_copy(c):
        return row_copy(cross, arrive, cross_send, cross_recv, {"ep": across}, c)

    def y_copy(c):
        return row_copy(y_out, out_ref, y_send, y_recv, {"pp": next_stage}, c)

    def combine(k, c, dst):
        info = meta_t[k, rows_of(c), :]
        col_ids = lax.broadcasted_iota(jnp.int32, (CHUNK, rows_owner), 1) + me * rows_owner
        col_ids = col_ids.astype(jnp.float32)
        weights = jnp.zeros((CHUNK, rows_owner), jnp.float32)
        for j in range(8):
            weights = weights + jnp.where(info[:, j:j + 1] == col_ids, info[:, 8 + j:9 + j], 0.0)
        high = weights.astype(jnp.bfloat16)
        rest = weights - high.astype(jnp.float32)
        middle = rest.astype(jnp.bfloat16)
        rest = rest - middle.astype(jnp.float32)
        pieces[0:CHUNK, :] = high
        pieces[CHUNK:2 * CHUNK, :] = middle
        pieces[2 * CHUNK:3 * CHUNK, :] = rest.astype(jnp.bfloat16)

        def one_tile(n, _):
            cols = pl.ds(pl.multiple_of(n * COLS, COLS), COLS)
            rows = tab[k, :, :, cols].reshape(rows_owner, COLS)
            prod = jnp.dot(pieces[...], rows, preferred_element_type=jnp.float32)
            dst[rows_of(c), cols] = prod[0:CHUNK] + prod[CHUNK:2 * CHUNK] + prod[2 * CHUNK:3 * CHUNK]
            return 0

        lax.fori_loop(0, dim // COLS, one_tile, 0)

    def loop(count, body):
        def step(i, _):
            body(i)
            return 0
        lax.fori_loop(0, count, step, 0)

    meta_t[3] = jnp.transpose(meta_ref[...])
    for k in range(3):
        meta_copy(k).wait_recv()
        meta_t[k] = jnp.transpose(meta_in[k])
    table_copy(0).wait()
    table_copy(1).wait()

    def send_diag(c):
        combine(0, c, diag_out)
        diag_copy(c).start()

    send_diag(0)
    send_diag(1)

    def send_cross(c):
        @pl.when(c + 2 < chunks)
        def _():
            send_diag(c + 2)
        combine(1, c, cross)
        diag_copy(c).wait_recv()
        cross[rows_of(c), :] = cross[rows_of(c), :] + diag_in[rows_of(c), :]
        cross_copy(c).start()

    loop(chunks, send_cross)
    table_copy(2).wait()

    def send_part(c):
        combine(2, c, part_out)
        part_copy(c).start()

    loop(chunks, send_part)
    table_copy(3).wait()
    loop(chunks, lambda c: combine(3, c, base))

    resid_copy().wait()

    def normalize(i):
        rows = pl.ds(pl.multiple_of(i * 16, 16), 16)
        normed[rows, :] = rms_norm(resid[rows, :], norm_ref[...]).astype(jnp.bfloat16)

    loop(tokens // 16, normalize)

    ff_tiles = ff_dim // ff_tile

    def gated(n):
        slot = n % 2
        gate_copy(n, slot).wait()
        up_copy(n, slot).wait()
        gate_act = jnp.dot(normed[...], w_gate[slot], preferred_element_type=jnp.float32)
        up_act = jnp.dot(normed[...], w_up[slot], preferred_element_type=jnp.float32)
        cols = pl.ds(pl.multiple_of(n * ff_tile, ff_tile), ff_tile)
        hidden[:, cols] = (jax.nn.silu(gate_act) * up_act).astype(jnp.bfloat16)

        @pl.when(n + 2 < ff_tiles)
        def _():
            gate_copy(n + 2, slot).start()
            up_copy(n + 2, slot).start()

    loop(ff_tiles, gated)
    loop(chunks, lambda c: part_copy(c).wait_recv())

    def project(n):
        slot = n % 2
        down_copy(n, slot).wait()
        shared = jnp.dot(hidden[...], w_down[slot], preferred_element_type=jnp.float32).astype(jnp.bfloat16)
        cols = pl.ds(pl.multiple_of(n * COLS, COLS), COLS)
        known = resid[:, cols].astype(jnp.float32) + shared.astype(jnp.float32)
        base[:, cols] = known + base[:, cols] + part_in[:, cols]

        @pl.when(n + 2 < dim // COLS)
        def _():
            down_copy(n + 2, slot).start()

    loop(dim // COLS, project)

    def finish(c):
        cross_copy(c).wait_recv()
        y_out[rows_of(c), :] = (base[rows_of(c), :] + arrive[rows_of(c), :]).astype(jnp.bfloat16)
        y_copy(c).start()

    loop(chunks, finish)

    for k in range(3):
        meta_copy(k).wait_send()

    def drain(c):
        diag_copy(c).wait_send()
        part_copy(c).wait_send()
        cross_copy(c).wait_send()
        y_copy(c).wait_send()
        y_copy(c).wait_recv()

    loop(chunks, drain)


def combine_stage(meta, expert_out, resid, norm_moe, w_gate, w_up, w_down):
    tokens, dim = resid.shape
    experts, slots_total, _ = expert_out.shape
    slots = slots_total // 4
    rows_owner = experts * slots
    ff_dim = w_gate.shape[1]
    chunks = tokens // CHUNK
    ff_tile = 256
    f32, bf16 = jnp.float32, jnp.bfloat16
    dma = pltpu.SemaphoreType.DMA
    vmem = pl.BlockSpec(memory_space=pltpu.VMEM)
    hbm = pl.BlockSpec(memory_space=pl.ANY)
    full = (tokens, dim)
    return pl.pallas_call(
        combine_kernel,
        out_shape=jax.ShapeDtypeStruct(full, bf16),
        in_specs=[vmem, hbm, hbm, vmem, hbm, hbm, hbm],
        out_specs=hbm,
        scratch_shapes=[
            pltpu.VMEM((4, experts, slots, dim), bf16),
            pltpu.VMEM((3,) + meta.shape, f32),
            pltpu.VMEM((4, meta.shape[1], meta.shape[0]), f32),
            pltpu.VMEM((3 * CHUNK, rows_owner), bf16),
            pltpu.VMEM(full, f32), pltpu.VMEM(full, f32), pltpu.VMEM(full, f32),
            pltpu.VMEM(full, f32), pltpu.VMEM(full, f32), pltpu.VMEM(full, f32), pltpu.VMEM(full, f32),
            pltpu.VMEM(full, bf16), pltpu.VMEM(full, bf16), pltpu.VMEM((tokens, ff_dim), bf16),
            pltpu.VMEM(full, bf16),
            pltpu.VMEM((2, dim, ff_tile), bf16), pltpu.VMEM((2, dim, ff_tile), bf16),
            pltpu.VMEM((2, ff_dim, COLS), bf16),
            dma((4,)), dma((3,)), dma((3,)),
            dma((chunks,)), dma((chunks,)), dma((chunks,)), dma((chunks,)),
            dma((chunks,)), dma((chunks,)), dma((chunks,)), dma((chunks,)),
            dma(()), dma((2,)), dma((2,)), dma((2,)),
        ],
        compiler_params=pltpu.CompilerParams(
            collective_id=0, has_side_effects=True, vmem_limit_bytes=62 * 1024 * 1024),
        name="combine_stage",
    )(meta, expert_out, resid, norm_moe, w_gate, w_up, w_down)


def attention_block(combined, norm_attn, w_query, w_key, w_value, w_out):
    seq_len = combined.shape[1]
    score_scale = 1.0 / math.sqrt(w_query.shape[2])
    normed = rms_norm(combined, norm_attn).astype(jnp.bfloat16)
    queries = jnp.einsum("bld,dhe->blhe", normed, w_query, preferred_element_type=jnp.float32).astype(jnp.bfloat16)
    key_heads = jnp.einsum("bld,dhe->blhe", normed, w_key, preferred_element_type=jnp.float32).astype(jnp.bfloat16)
    value_heads = jnp.einsum("bld,dhe->blhe", normed, w_value, preferred_element_type=jnp.float32).astype(jnp.bfloat16)
    scores = jnp.einsum("bqhe,bkhe->bhqk", queries, key_heads, preferred_element_type=jnp.float32) * score_scale
    causal = jnp.arange(seq_len)[:, None] >= jnp.arange(seq_len)[None, :]
    scores = jnp.where(causal, scores, -1e30)
    attn_probs = jnp.exp(scores - jnp.max(scores, axis=-1, keepdims=True))
    prob_sum = jnp.sum(attn_probs, axis=-1, keepdims=True)
    attn_mixed = jnp.einsum("bhqk,bkhe->bhqe", attn_probs.astype(jnp.bfloat16), value_heads, preferred_element_type=jnp.float32) / prob_sum
    attn_proj = jnp.einsum("cirf,ife->cre", attn_mixed.astype(jnp.bfloat16), w_out, preferred_element_type=jnp.float32).astype(jnp.bfloat16)
    return (combined.astype(jnp.float32) + attn_proj.astype(jnp.float32)).astype(jnp.bfloat16)


def solution(mesh):
    ep_size = mesh.shape["ep"]
    tok_spec = P("pp", "data", "ep", None, None)
    vec_spec = P("pp", None)
    mat_spec = P("pp", None, None)
    head_spec = P("pp", None, None, None)

    def device_step(expert_out, expert_ids, slot_ids, gate_weights, residual, norm_moe, w_gate, w_up, w_down, norm_attn, w_query, w_key, w_value, w_out):
        seqs, seq_len, top_k = expert_ids.shape[2:]
        tokens = seqs * seq_len
        dim = residual.shape[-1]
        cap_slots = expert_out.shape[3] // ep_size
        first_slot = lax.axis_index("ep") * cap_slots
        slot_here = slot_ids[0, 0]
        kept_mask = slot_here >= 0
        col_ids = jnp.where(kept_mask, expert_ids[0, 0] * cap_slots + slot_here - first_slot, -1)
        weights = jnp.where(kept_mask, gate_weights[0, 0], 0.0)
        meta = jnp.concatenate([col_ids.astype(jnp.float32), weights], axis=-1).reshape(tokens, 2 * top_k)
        meta = jnp.pad(meta.T, ((0, 0), (0, 256 - tokens)))
        incoming = combine_stage(
            meta, expert_out[0, 0], residual.reshape(tokens, dim), norm_moe, w_gate[0], w_up[0], w_down[0])
        incoming = incoming.reshape(seqs, seq_len, dim)
        result = attention_block(incoming, norm_attn[0], w_query[0], w_key[0], w_value[0], w_out[0])
        return result[None, None]

    in_specs = (tok_spec,) * 5 + (vec_spec, mat_spec, mat_spec, mat_spec, vec_spec, head_spec, head_spec, head_spec, head_spec)
    return jax.shard_map(device_step, mesh=mesh, in_specs=in_specs, out_specs=tok_spec, check_vma=False)
```

```python
import math
import functools
import jax
import jax.numpy as jnp
from jax import lax
from jax.experimental import pallas as pl
from jax.experimental.pallas import tpu as pltpu
from jax.sharding import PartitionSpec as P

EPSILON = 1e-6
MESH = pl.DeviceIdType.MESH
CHUNK = 32
COLS = 512
WIDE = 2048


def rms_norm(tensor, gain):
    values = tensor.astype(jnp.float32)
    inv_rms = lax.rsqrt(jnp.mean(values * values, axis=-1, keepdims=True) + EPSILON)
    return values * inv_rms * gain


def combine_kernel(
    meta_ref, expert_ref, resid_hbm, norm_ref, gate_hbm, up_hbm, down_hbm, out_ref,
    tab, meta_in, meta_t, pieces, diag_out, diag_in, cross, part_out, part_in, arrive, base,
    resid, normed, hidden, y_out, w_gate, w_up, w_down,
    tab_sem, meta_send, meta_recv, diag_send, diag_recv, part_send, part_recv,
    cross_send, cross_recv, y_send, y_recv, resid_sem, gate_sem, up_sem, down_sem,
):
    tokens, dim = resid.shape
    chunks = tokens // CHUNK
    rows_owner = tab.shape[1] * tab.shape[2]
    slots = tab.shape[2]
    ff_dim = hidden.shape[1]
    me = lax.axis_index("ep")
    stage = lax.axis_index("pp")
    y_pos, core = me // 2, me % 2
    pair = y_pos * 2 + (1 - core)
    across = (1 - y_pos) * 2 + core
    diagonal = (1 - y_pos) * 2 + (1 - core)
    next_stage, prev_stage = (stage + 1) % 4, (stage + 3) % 4

    owners = (diagonal, across, pair, me)

    def table_copy(k):
        start = pl.multiple_of(owners[k] * slots, slots)
        return pltpu.make_async_copy(expert_ref.at[:, pl.ds(start, slots), :], tab.at[k], tab_sem.at[k])

    def resid_copy():
        return pltpu.make_async_copy(resid_hbm, resid, resid_sem)

    ff_tile = w_gate.shape[2]

    def gate_copy(n, slot):
        cols = pl.ds(pl.multiple_of(n * ff_tile, ff_tile), ff_tile)
        return pltpu.make_async_copy(gate_hbm.at[:, cols], w_gate.at[slot], gate_sem.at[slot])

    def up_copy(n, slot):
        cols = pl.ds(pl.multiple_of(n * ff_tile, ff_tile), ff_tile)
        return pltpu.make_async_copy(up_hbm.at[:, cols], w_up.at[slot], up_sem.at[slot])

    def down_copy(n, slot):
        cols = pl.ds(pl.multiple_of(n * COLS, COLS), COLS)
        return pltpu.make_async_copy(down_hbm.at[:, cols], w_down.at[slot], down_sem.at[slot])

    for k in range(4):
        table_copy(k).start()
    resid_copy().start()
    for slot in range(2):
        gate_copy(slot, slot).start()
        up_copy(slot, slot).start()
        down_copy(slot, slot).start()

    barrier = pltpu.get_barrier_semaphore()
    for peer in (pair, across, diagonal):
        pl.semaphore_signal(barrier, inc=1, device_id={"ep": peer}, device_id_type=MESH)
    for peer in (next_stage, prev_stage):
        pl.semaphore_signal(barrier, inc=1, device_id={"pp": peer}, device_id_type=MESH)
    pl.semaphore_wait(barrier, 5)

    def meta_copy(k):
        return pltpu.make_async_remote_copy(
            src_ref=meta_ref, dst_ref=meta_in.at[k], send_sem=meta_send.at[k], recv_sem=meta_recv.at[k],
            device_id={"ep": owners[k]}, device_id_type=MESH)

    for k in range(3):
        meta_copy(k).start()

    def rows_of(c):
        return pl.ds(pl.multiple_of(c * CHUNK, CHUNK), CHUNK)

    def row_copy(src, dst, send, recv, target, c):
        return pltpu.make_async_remote_copy(
            src_ref=src.at[rows_of(c), :], dst_ref=dst.at[rows_of(c), :], send_sem=send.at[c], recv_sem=recv.at[c],
            device_id=target, device_id_type=MESH)

    def diag_copy(c):
        return row_copy(diag_out, diag_in, diag_send, diag_recv, {"ep": pair}, c)

    def part_copy(c):
        return row_copy(part_out, part_in, part_send, part_recv, {"ep": pair}, c)

    def cross_copy(c):
        return row_copy(cross, arrive, cross_send, cross_recv, {"ep": across}, c)

    def y_copy(c):
        return row_copy(y_out, out_ref, y_send, y_recv, {"pp": next_stage}, c)

    def combine(k, c, dst):
        info = meta_t[k, rows_of(c), :]
        col_ids = lax.broadcasted_iota(jnp.int32, (CHUNK, rows_owner), 1) + me * rows_owner
        col_ids = col_ids.astype(jnp.float32)
        weights = jnp.zeros((CHUNK, rows_owner), jnp.float32)
        for j in range(8):
            weights = weights + jnp.where(info[:, j:j + 1] == col_ids, info[:, 8 + j:9 + j], 0.0)
        high = weights.astype(jnp.bfloat16)
        rest = weights - high.astype(jnp.float32)
        middle = rest.astype(jnp.bfloat16)
        rest = rest - middle.astype(jnp.float32)
        pieces[0:CHUNK, :] = high
        pieces[CHUNK:2 * CHUNK, :] = middle
        pieces[2 * CHUNK:3 * CHUNK, :] = rest.astype(jnp.bfloat16)

        def one_tile(n, _):
            cols = pl.ds(pl.multiple_of(n * WIDE, WIDE), WIDE)
            rows = tab[k, :, :, cols].reshape(rows_owner, WIDE)
            prod = jnp.dot(pieces[...], rows, preferred_element_type=jnp.float32)
            dst[rows_of(c), cols] = prod[0:CHUNK] + prod[CHUNK:2 * CHUNK] + prod[2 * CHUNK:3 * CHUNK]
            return 0

        lax.fori_loop(0, dim // WIDE, one_tile, 0)

    def loop(count, body):
        def step(i, _):
            body(i)
            return 0
        lax.fori_loop(0, count, step, 0)

    meta_t[3] = jnp.transpose(meta_ref[...])
    for k in range(3):
        meta_copy(k).wait_recv()
        meta_t[k] = jnp.transpose(meta_in[k])
    table_copy(0).wait()
    table_copy(1).wait()

    def send_diag(c):
        combine(0, c, diag_out)
        diag_copy(c).start()

    send_diag(0)
    send_diag(1)

    def send_cross(c):
        @pl.when(c + 2 < chunks)
        def _():
            send_diag(c + 2)
        combine(1, c, cross)
        diag_copy(c).wait_recv()
        cross[rows_of(c), :] = cross[rows_of(c), :] + diag_in[rows_of(c), :]
        cross_copy(c).start()

    loop(chunks, send_cross)
    table_copy(2).wait()

    def send_part(c):
        combine(2, c, part_out)
        part_copy(c).start()

    loop(chunks, send_part)
    table_copy(3).wait()
    loop(chunks, lambda c: combine(3, c, base))

    resid_copy().wait()

    def normalize(i):
        rows = pl.ds(pl.multiple_of(i * 16, 16), 16)
        normed[rows, :] = rms_norm(resid[rows, :], norm_ref[...]).astype(jnp.bfloat16)

    loop(tokens // 16, normalize)

    ff_tiles = ff_dim // ff_tile

    def gated(n):
        slot = n % 2
        gate_copy(n, slot).wait()
        up_copy(n, slot).wait()
        gate_act = jnp.dot(normed[...], w_gate[slot], preferred_element_type=jnp.float32)
        up_act = jnp.dot(normed[...], w_up[slot], preferred_element_type=jnp.float32)
        cols = pl.ds(pl.multiple_of(n * ff_tile, ff_tile), ff_tile)
        hidden[:, cols] = (jax.nn.silu(gate_act) * up_act).astype(jnp.bfloat16)

        @pl.when(n + 2 < ff_tiles)
        def _():
            gate_copy(n + 2, slot).start()
            up_copy(n + 2, slot).start()

    loop(ff_tiles, gated)
    loop(chunks, lambda c: part_copy(c).wait_recv())

    def project(n):
        slot = n % 2
        down_copy(n, slot).wait()
        shared = jnp.dot(hidden[...], w_down[slot], preferred_element_type=jnp.float32).astype(jnp.bfloat16)
        cols = pl.ds(pl.multiple_of(n * COLS, COLS), COLS)
        known = resid[:, cols].astype(jnp.float32) + shared.astype(jnp.float32)
        base[:, cols] = known + base[:, cols] + part_in[:, cols]

        @pl.when(n + 2 < dim // COLS)
        def _():
            down_copy(n + 2, slot).start()

    loop(dim // COLS, project)

    def finish(c):
        cross_copy(c).wait_recv()
        y_out[rows_of(c), :] = (base[rows_of(c), :] + arrive[rows_of(c), :]).astype(jnp.bfloat16)
        y_copy(c).start()

    loop(chunks, finish)

    for k in range(3):
        meta_copy(k).wait_send()

    def drain(c):
        diag_copy(c).wait_send()
        part_copy(c).wait_send()
        cross_copy(c).wait_send()
        y_copy(c).wait_send()
        y_copy(c).wait_recv()

    loop(chunks, drain)


def combine_stage(meta, expert_out, resid, norm_moe, w_gate, w_up, w_down):
    tokens, dim = resid.shape
    experts, slots_total, _ = expert_out.shape
    slots = slots_total // 4
    rows_owner = experts * slots
    ff_dim = w_gate.shape[1]
    chunks = tokens // CHUNK
    ff_tile = 256
    f32, bf16 = jnp.float32, jnp.bfloat16
    dma = pltpu.SemaphoreType.DMA
    vmem = pl.BlockSpec(memory_space=pltpu.VMEM)
    hbm = pl.BlockSpec(memory_space=pl.ANY)
    full = (tokens, dim)
    return pl.pallas_call(
        combine_kernel,
        out_shape=jax.ShapeDtypeStruct(full, bf16),
        in_specs=[vmem, hbm, hbm, vmem, hbm, hbm, hbm],
        out_specs=hbm,
        scratch_shapes=[
            pltpu.VMEM((4, experts, slots, dim), bf16),
            pltpu.VMEM((3,) + meta.shape, f32),
            pltpu.VMEM((4, meta.shape[1], meta.shape[0]), f32),
            pltpu.VMEM((3 * CHUNK, rows_owner), bf16),
            pltpu.VMEM(full, f32), pltpu.VMEM(full, f32), pltpu.VMEM(full, f32),
            pltpu.VMEM(full, f32), pltpu.VMEM(full, f32), pltpu.VMEM(full, f32), pltpu.VMEM(full, f32),
            pltpu.VMEM(full, bf16), pltpu.VMEM(full, bf16), pltpu.VMEM((tokens, ff_dim), bf16),
            pltpu.VMEM(full, bf16),
            pltpu.VMEM((2, dim, ff_tile), bf16), pltpu.VMEM((2, dim, ff_tile), bf16),
            pltpu.VMEM((2, ff_dim, COLS), bf16),
            dma((4,)), dma((3,)), dma((3,)),
            dma((chunks,)), dma((chunks,)), dma((chunks,)), dma((chunks,)),
            dma((chunks,)), dma((chunks,)), dma((chunks,)), dma((chunks,)),
            dma(()), dma((2,)), dma((2,)), dma((2,)),
        ],
        compiler_params=pltpu.CompilerParams(
            collective_id=0, has_side_effects=True, vmem_limit_bytes=62 * 1024 * 1024),
        name="combine_stage",
    )(meta, expert_out, resid, norm_moe, w_gate, w_up, w_down)


def attention_kernel(
    seq_len, y_hbm, gain_ref, query_hbm, key_hbm, value_hbm, out_w_hbm, out_hbm,
    y_in, normed, w_heads, w_cols, heads_qkv, mixed, out_tile,
    y_sem, head_sem, col_sem, out_sem,
):
    tokens, dim = y_in.shape
    group = w_heads.shape[2]
    head_dim = w_heads.shape[3]
    width = group * head_dim
    groups = mixed.shape[1] // width
    tile = w_cols.shape[2]
    weights = (query_hbm, key_hbm, value_hbm)

    def head_copy(g, i):
        heads = pl.ds(pl.multiple_of(g * group, group), group)
        return pltpu.make_async_copy(weights[i].at[:, heads, :], w_heads.at[i], head_sem.at[i])

    def col_copy(n, slot):
        cols = pl.ds(pl.multiple_of(n * tile, tile), tile)
        return pltpu.make_async_copy(out_w_hbm.at[:, cols], w_cols.at[slot], col_sem.at[slot])

    def out_copy(n, slot):
        cols = pl.ds(pl.multiple_of(n * tile, tile), tile)
        return pltpu.make_async_copy(out_tile.at[slot], out_hbm.at[:, cols], out_sem.at[slot])

    def loop(count, body):
        def step(i, _):
            body(i)
            return 0
        lax.fori_loop(0, count, step, 0)

    y_copy = pltpu.make_async_copy(y_hbm, y_in, y_sem)
    y_copy.start()
    head_copy(0, 0).start()
    head_copy(0, 1).start()
    y_copy.wait()

    def normalize(i):
        rows = pl.ds(pl.multiple_of(i * 16, 16), 16)
        normed[rows, :] = rms_norm(y_in[rows, :], gain_ref[...]).astype(jnp.bfloat16)

    loop(tokens // 16, normalize)

    query_pos = lax.broadcasted_iota(jnp.int32, (tokens, tokens), 0)
    key_pos = lax.broadcasted_iota(jnp.int32, (tokens, tokens), 1)
    visible = (query_pos >= key_pos) & (query_pos // seq_len == key_pos // seq_len)
    score_scale = 1.0 / math.sqrt(head_dim)

    def one_group(g):
        for i in range(3):
            head_copy(g, i).wait()
            if i == 0:
                head_copy(g, 2).start()
            else:
                @pl.when(g + 1 < groups)
                def _():
                    head_copy(g + 1, i - 1).start()
            if i == 2:
                @pl.when(g == groups - 1)
                def _():
                    col_copy(0, 0).start()
                    col_copy(1, 1).start()
            flat = w_heads[i].reshape(dim, width)
            heads_qkv[i] = jnp.dot(normed[...], flat, preferred_element_type=jnp.float32).astype(jnp.bfloat16)
        for h in range(group):
            cols = slice(h * head_dim, (h + 1) * head_dim)
            scores = lax.dot_general(
                heads_qkv[0, :, cols], heads_qkv[1, :, cols], (((1,), (1,)), ((), ())),
                preferred_element_type=jnp.float32) * score_scale
            scores = jnp.where(visible, scores, -1e30)
            probs = jnp.exp(scores - jnp.max(scores, axis=-1, keepdims=True))
            prob_sum = jnp.sum(probs, axis=-1, keepdims=True)
            head_out = jnp.dot(
                probs.astype(jnp.bfloat16), heads_qkv[2, :, cols], preferred_element_type=jnp.float32) / prob_sum
            start = pl.multiple_of(g * width + h * head_dim, head_dim)
            mixed[:, pl.ds(start, head_dim)] = head_out.astype(jnp.bfloat16)

    loop(groups, one_group)

    tiles = dim // tile

    def project(n):
        slot = n % 2
        col_copy(n, slot).wait()

        @pl.when(n >= 2)
        def _():
            out_copy(n - 2, slot).wait()
        proj = jnp.dot(mixed[...], w_cols[slot], preferred_element_type=jnp.float32).astype(jnp.bfloat16)
        cols = pl.ds(pl.multiple_of(n * tile, tile), tile)
        out_tile[slot] = (y_in[:, cols].astype(jnp.float32) + proj.astype(jnp.float32)).astype(jnp.bfloat16)
        out_copy(n, slot).start()

        @pl.when(n + 2 < tiles)
        def _():
            col_copy(n + 2, slot).start()

    loop(tiles, project)
    for n in range(tiles - 2, tiles):
        out_copy(n, n % 2).wait()


def attention_stage(seq_len, incoming, norm_attn, w_query, w_key, w_value, w_out):
    tokens, dim = incoming.shape
    heads, head_dim = w_query.shape[1:]
    group = 8
    tile = 1024
    bf16 = jnp.bfloat16
    dma = pltpu.SemaphoreType.DMA
    vmem = pl.BlockSpec(memory_space=pltpu.VMEM)
    hbm = pl.BlockSpec(memory_space=pl.ANY)
    return pl.pallas_call(
        functools.partial(attention_kernel, seq_len),
        out_shape=jax.ShapeDtypeStruct((tokens, dim), bf16),
        in_specs=[hbm, vmem, hbm, hbm, hbm, hbm],
        out_specs=hbm,
        scratch_shapes=[
            pltpu.VMEM((tokens, dim), bf16), pltpu.VMEM((tokens, dim), bf16),
            pltpu.VMEM((3, dim, group, head_dim), bf16), pltpu.VMEM((2, heads * head_dim, tile), bf16),
            pltpu.VMEM((3, tokens, group * head_dim), bf16), pltpu.VMEM((tokens, heads * head_dim), bf16),
            pltpu.VMEM((2, tokens, tile), bf16),
            dma(()), dma((3,)), dma((2,)), dma((2,)),
        ],
        compiler_params=pltpu.CompilerParams(vmem_limit_bytes=62 * 1024 * 1024),
        name="attention_stage",
    )(incoming, norm_attn, w_query, w_key, w_value, w_out.reshape(heads * head_dim, dim))


def solution(mesh):
    ep_size = mesh.shape["ep"]
    tok_spec = P("pp", "data", "ep", None, None)
    vec_spec = P("pp", None)
    mat_spec = P("pp", None, None)
    head_spec = P("pp", None, None, None)

    def device_step(expert_out, expert_ids, slot_ids, gate_weights, residual, norm_moe, w_gate, w_up, w_down, norm_attn, w_query, w_key, w_value, w_out):
        seqs, seq_len, top_k = expert_ids.shape[2:]
        tokens = seqs * seq_len
        dim = residual.shape[-1]
        cap_slots = expert_out.shape[3] // ep_size
        first_slot = lax.axis_index("ep") * cap_slots
        slot_here = slot_ids[0, 0]
        kept_mask = slot_here >= 0
        col_ids = jnp.where(kept_mask, expert_ids[0, 0] * cap_slots + slot_here - first_slot, -1)
        weights = jnp.where(kept_mask, gate_weights[0, 0], 0.0)
        meta = jnp.concatenate([col_ids.astype(jnp.float32), weights], axis=-1).reshape(tokens, 2 * top_k)
        meta = jnp.pad(meta.T, ((0, 0), (0, 256 - tokens)))
        incoming = combine_stage(
            meta, expert_out[0, 0], residual.reshape(tokens, dim), norm_moe, w_gate[0], w_up[0], w_down[0])
        result = attention_stage(seq_len, incoming, norm_attn, w_query[0], w_key[0], w_value[0], w_out[0])
        return result.reshape(1, 1, seqs, seq_len, dim)

    in_specs = (tok_spec,) * 5 + (vec_spec, mat_spec, mat_spec, mat_spec, vec_spec, head_spec, head_spec, head_spec, head_spec)
    return jax.shard_map(device_step, mesh=mesh, in_specs=in_specs, out_specs=tok_spec, check_vma=False)
```

```python
import math
import functools
import jax
import jax.numpy as jnp
from jax import lax
from jax.experimental import pallas as pl
from jax.experimental.pallas import tpu as pltpu
from jax.sharding import PartitionSpec as P

EPSILON = 1e-6
MESH = pl.DeviceIdType.MESH
CHUNK = 32
PART = 16
COLS = 512
WIDE = 2048


def rms_norm(tensor, gain):
    values = tensor.astype(jnp.float32)
    inv_rms = lax.rsqrt(jnp.mean(values * values, axis=-1, keepdims=True) + EPSILON)
    return values * inv_rms * gain


def combine_kernel(
    meta_ref, expert_ref, resid_hbm, norm_ref, gate_hbm, up_hbm, down_hbm, out_ref,
    tab, meta_in, meta_t, pieces, diag_out, diag_in, cross, part_out, part_in, arrive, base,
    resid, normed, hidden, y_out, y_in, w_gate, w_up, w_down,
    tab_sem, meta_send, meta_recv, diag_send, diag_recv, part_send, part_recv,
    cross_send, cross_recv, y_send, y_recv, pair_send, pair_recv, keep_sem, resid_sem, gate_sem, up_sem, down_sem,
):
    tokens, dim = resid.shape
    chunks = tokens // CHUNK
    parts = tokens // PART
    rows_owner = tab.shape[1] * tab.shape[2]
    slots = tab.shape[2]
    ff_dim = hidden.shape[1]
    me = lax.axis_index("ep")
    stage = lax.axis_index("pp")
    y_pos, core = me // 2, me % 2
    pair = y_pos * 2 + (1 - core)
    across = (1 - y_pos) * 2 + core
    diagonal = (1 - y_pos) * 2 + (1 - core)
    next_stage, prev_stage = (stage + 1) % 4, (stage + 3) % 4

    owners = (diagonal, across, pair, me)

    def table_copy(k):
        start = pl.multiple_of(owners[k] * slots, slots)
        return pltpu.make_async_copy(expert_ref.at[:, pl.ds(start, slots), :], tab.at[k], tab_sem.at[k])

    def resid_copy():
        return pltpu.make_async_copy(resid_hbm, resid, resid_sem)

    ff_tile = w_gate.shape[2]

    def gate_copy(n, slot):
        cols = pl.ds(pl.multiple_of(n * ff_tile, ff_tile), ff_tile)
        return pltpu.make_async_copy(gate_hbm.at[:, cols], w_gate.at[slot], gate_sem.at[slot])

    def up_copy(n, slot):
        cols = pl.ds(pl.multiple_of(n * ff_tile, ff_tile), ff_tile)
        return pltpu.make_async_copy(up_hbm.at[:, cols], w_up.at[slot], up_sem.at[slot])

    def down_copy(n, slot):
        cols = pl.ds(pl.multiple_of(n * COLS, COLS), COLS)
        return pltpu.make_async_copy(down_hbm.at[:, cols], w_down.at[slot], down_sem.at[slot])

    for k in range(4):
        table_copy(k).start()
    resid_copy().start()
    for slot in range(2):
        gate_copy(slot, slot).start()
        up_copy(slot, slot).start()
        down_copy(slot, slot).start()

    barrier = pltpu.get_barrier_semaphore()
    for peer in (pair, across, diagonal):
        pl.semaphore_signal(barrier, inc=1, device_id={"ep": peer}, device_id_type=MESH)
    for peer in (next_stage, prev_stage):
        pl.semaphore_signal(barrier, inc=1, device_id={"pp": peer}, device_id_type=MESH)
    pl.semaphore_wait(barrier, 5)

    def meta_copy(k):
        return pltpu.make_async_remote_copy(
            src_ref=meta_ref, dst_ref=meta_in.at[k], send_sem=meta_send.at[k], recv_sem=meta_recv.at[k],
            device_id={"ep": owners[k]}, device_id_type=MESH)

    for k in range(3):
        meta_copy(k).start()

    def rows_of(c):
        return pl.ds(pl.multiple_of(c * CHUNK, CHUNK), CHUNK)

    def row_copy(src, dst, send, recv, target, c):
        return pltpu.make_async_remote_copy(
            src_ref=src.at[rows_of(c), :], dst_ref=dst.at[rows_of(c), :], send_sem=send.at[c], recv_sem=recv.at[c],
            device_id=target, device_id_type=MESH)

    def diag_copy(c):
        return row_copy(diag_out, diag_in, diag_send, diag_recv, {"ep": pair}, c)

    def part_copy(c):
        return row_copy(part_out, part_in, part_send, part_recv, {"ep": pair}, c)

    def rows_of_part(c):
        return pl.ds(pl.multiple_of(c * PART, PART), PART)

    def part_row_copy(src, dst, send, recv, target, c):
        return pltpu.make_async_remote_copy(
            src_ref=src.at[rows_of_part(c), :], dst_ref=dst.at[rows_of_part(c), :],
            send_sem=send.at[c], recv_sem=recv.at[c], device_id=target, device_id_type=MESH)

    def cross_copy(c):
        return part_row_copy(cross, arrive, cross_send, cross_recv, {"ep": across}, c)

    def y_copy(c):
        return part_row_copy(y_out, y_in, y_send, y_recv, {"pp": next_stage}, c)

    def pair_copy(c):
        return part_row_copy(y_in, out_ref.at[core], pair_send, pair_recv, {"ep": pair}, c)

    def keep_copy(c):
        rows = rows_of_part(c)
        return pltpu.make_async_copy(y_in.at[rows, :], out_ref.at[core, rows, :], keep_sem.at[c])

    def combine(k, c, dst):
        info = meta_t[k, rows_of(c), :]
        col_ids = lax.broadcasted_iota(jnp.int32, (CHUNK, rows_owner), 1) + me * rows_owner
        col_ids = col_ids.astype(jnp.float32)
        weights = jnp.zeros((CHUNK, rows_owner), jnp.float32)
        for j in range(8):
            weights = weights + jnp.where(info[:, j:j + 1] == col_ids, info[:, 8 + j:9 + j], 0.0)
        high = weights.astype(jnp.bfloat16)
        rest = weights - high.astype(jnp.float32)
        middle = rest.astype(jnp.bfloat16)
        rest = rest - middle.astype(jnp.float32)
        pieces[0:CHUNK, :] = high
        pieces[CHUNK:2 * CHUNK, :] = middle
        pieces[2 * CHUNK:3 * CHUNK, :] = rest.astype(jnp.bfloat16)

        def one_tile(n, _):
            cols = pl.ds(pl.multiple_of(n * WIDE, WIDE), WIDE)
            rows = tab[k, :, :, cols].reshape(rows_owner, WIDE)
            prod = jnp.dot(pieces[...], rows, preferred_element_type=jnp.float32)
            dst[rows_of(c), cols] = prod[0:CHUNK] + prod[CHUNK:2 * CHUNK] + prod[2 * CHUNK:3 * CHUNK]
            return 0

        lax.fori_loop(0, dim // WIDE, one_tile, 0)

    def loop(count, body):
        def step(i, _):
            body(i)
            return 0
        lax.fori_loop(0, count, step, 0)

    meta_t[3] = jnp.transpose(meta_ref[...])
    for k in range(3):
        meta_copy(k).wait_recv()
        meta_t[k] = jnp.transpose(meta_in[k])
    table_copy(0).wait()
    table_copy(1).wait()

    def send_diag(c):
        combine(0, c, diag_out)
        diag_copy(c).start()

    send_diag(0)
    send_diag(1)

    def send_cross(c):
        @pl.when(c + 2 < chunks)
        def _():
            send_diag(c + 2)
        combine(1, c, cross)
        diag_copy(c).wait_recv()
        cross[rows_of(c), :] = cross[rows_of(c), :] + diag_in[rows_of(c), :]
        for i in range(CHUNK // PART):
            cross_copy(c * (CHUNK // PART) + i).start()

    loop(chunks, send_cross)
    table_copy(2).wait()

    def send_part(c):
        combine(2, c, part_out)
        part_copy(c).start()

    loop(chunks, send_part)
    table_copy(3).wait()
    loop(chunks, lambda c: combine(3, c, base))

    resid_copy().wait()

    def normalize(i):
        rows = pl.ds(pl.multiple_of(i * 16, 16), 16)
        normed[rows, :] = rms_norm(resid[rows, :], norm_ref[...]).astype(jnp.bfloat16)

    loop(tokens // 16, normalize)

    ff_tiles = ff_dim // ff_tile

    def gated(n):
        slot = n % 2
        gate_copy(n, slot).wait()
        up_copy(n, slot).wait()
        gate_act = jnp.dot(normed[...], w_gate[slot], preferred_element_type=jnp.float32)
        up_act = jnp.dot(normed[...], w_up[slot], preferred_element_type=jnp.float32)
        cols = pl.ds(pl.multiple_of(n * ff_tile, ff_tile), ff_tile)
        hidden[:, cols] = (jax.nn.silu(gate_act) * up_act).astype(jnp.bfloat16)

        @pl.when(n + 2 < ff_tiles)
        def _():
            gate_copy(n + 2, slot).start()
            up_copy(n + 2, slot).start()

    loop(ff_tiles, gated)
    loop(chunks, lambda c: part_copy(c).wait_recv())

    def project(n):
        slot = n % 2
        down_copy(n, slot).wait()
        shared = jnp.dot(hidden[...], w_down[slot], preferred_element_type=jnp.float32).astype(jnp.bfloat16)
        cols = pl.ds(pl.multiple_of(n * COLS, COLS), COLS)
        known = resid[:, cols].astype(jnp.float32) + shared.astype(jnp.float32)
        base[:, cols] = known + base[:, cols] + part_in[:, cols]

        @pl.when(n + 2 < dim // COLS)
        def _():
            down_copy(n + 2, slot).start()

    loop(dim // COLS, project)

    def finish(c):
        rows = rows_of_part(c)
        cross_copy(c).wait_recv()
        y_out[rows, :] = (base[rows, :] + arrive[rows, :]).astype(jnp.bfloat16)
        y_copy(c).start()

    def spread(c):
        y_copy(c).wait_recv()
        pair_copy(c).start()
        keep_copy(c).start()

    def finish_and_spread(c):
        finish(c + 1)
        spread(c)

    finish(0)
    loop(parts - 1, finish_and_spread)
    spread(parts - 1)

    for k in range(3):
        meta_copy(k).wait_send()

    def drain(c):
        diag_copy(c).wait_send()
        part_copy(c).wait_send()

    loop(chunks, drain)

    def drain_parts(c):
        cross_copy(c).wait_send()
        y_copy(c).wait_send()
        pair_copy(c).wait_send()
        pair_copy(c).wait_recv()
        keep_copy(c).wait()

    loop(parts, drain_parts)


def combine_stage(meta, expert_out, resid, norm_moe, w_gate, w_up, w_down):
    tokens, dim = resid.shape
    experts, slots_total, _ = expert_out.shape
    slots = slots_total // 4
    rows_owner = experts * slots
    ff_dim = w_gate.shape[1]
    chunks = tokens // CHUNK
    parts = tokens // PART
    ff_tile = 256
    f32, bf16 = jnp.float32, jnp.bfloat16
    dma = pltpu.SemaphoreType.DMA
    vmem = pl.BlockSpec(memory_space=pltpu.VMEM)
    hbm = pl.BlockSpec(memory_space=pl.ANY)
    full = (tokens, dim)
    return pl.pallas_call(
        combine_kernel,
        out_shape=jax.ShapeDtypeStruct((2,) + full, bf16),
        in_specs=[vmem, hbm, hbm, vmem, hbm, hbm, hbm],
        out_specs=hbm,
        scratch_shapes=[
            pltpu.VMEM((4, experts, slots, dim), bf16),
            pltpu.VMEM((3,) + meta.shape, f32),
            pltpu.VMEM((4, meta.shape[1], meta.shape[0]), f32),
            pltpu.VMEM((3 * CHUNK, rows_owner), bf16),
            pltpu.VMEM(full, f32), pltpu.VMEM(full, f32), pltpu.VMEM(full, f32),
            pltpu.VMEM(full, f32), pltpu.VMEM(full, f32), pltpu.VMEM(full, f32), pltpu.VMEM(full, f32),
            pltpu.VMEM(full, bf16), pltpu.VMEM(full, bf16), pltpu.VMEM((tokens, ff_dim), bf16),
            pltpu.VMEM(full, bf16), pltpu.VMEM(full, bf16),
            pltpu.VMEM((2, dim, ff_tile), bf16), pltpu.VMEM((2, dim, ff_tile), bf16),
            pltpu.VMEM((2, ff_dim, COLS), bf16),
            dma((4,)), dma((3,)), dma((3,)),
            dma((chunks,)), dma((chunks,)), dma((chunks,)), dma((chunks,)),
            dma((parts,)), dma((parts,)), dma((parts,)), dma((parts,)),
            dma((parts,)), dma((parts,)), dma((parts,)),
            dma(()), dma((2,)), dma((2,)), dma((2,)),
        ],
        compiler_params=pltpu.CompilerParams(
            collective_id=0, has_side_effects=True, vmem_limit_bytes=62 * 1024 * 1024),
        name="combine_stage",
    )(meta, expert_out, resid, norm_moe, w_gate, w_up, w_down)


def attention_kernel(
    seq_len, y_hbm, gain_ref, query_hbm, key_hbm, value_hbm, out_w_hbm, out_hbm,
    y_in, normed, w_heads, w_cols, heads_qkv, mixed_own, mixed_out, mixed_in, out_tile,
    y_sem, head_sem, col_sem, out_sem, mixed_send, mixed_recv,
):
    _, tokens, dim = y_hbm.shape
    group, head_dim = w_heads.shape[2:]
    width = group * head_dim
    groups = mixed_own.shape[1] // width
    half = groups * width
    tile = w_cols.shape[2]
    tiles = dim // tile
    weights = (query_hbm, key_hbm, value_hbm)
    me = lax.axis_index("ep")
    core = me % 2
    pair = (me // 2) * 2 + (1 - core)

    def head_copy(g, i):
        heads = pl.ds(pl.multiple_of((core * groups + g) * group, group), group)
        return pltpu.make_async_copy(weights[i].at[:, heads, :], w_heads.at[i], head_sem.at[i])

    def col_copies(n, slot):
        cols = pl.ds(pl.multiple_of(n * tile, tile), tile)
        own = pl.ds(pl.multiple_of(core * half, half), half)
        other = pl.ds(pl.multiple_of((1 - core) * half, half), half)
        return (
            pltpu.make_async_copy(out_w_hbm.at[own, cols], w_cols.at[slot, 0:half], col_sem.at[slot, 0]),
            pltpu.make_async_copy(out_w_hbm.at[other, cols], w_cols.at[slot, half:2 * half], col_sem.at[slot, 1]))

    def col_start(n, slot):
        for copy in col_copies(n, slot):
            copy.start()

    def out_copy(n, slot):
        cols = pl.ds(pl.multiple_of(n * tile, tile), tile)
        return pltpu.make_async_copy(out_tile.at[slot], out_hbm.at[:, cols], out_sem.at[slot])

    def mixed_copy(g):
        cols = pl.ds(g * width, width)
        return pltpu.make_async_remote_copy(
            src_ref=mixed_out.at[:, cols], dst_ref=mixed_in.at[:, cols], send_sem=mixed_send.at[g],
            recv_sem=mixed_recv.at[g], device_id={"ep": pair}, device_id_type=MESH)

    def loop(count, body):
        def step(i, _):
            body(i)
            return 0
        lax.fori_loop(0, count, step, 0)

    y_copies = [pltpu.make_async_copy(y_hbm.at[b], y_in.at[pl.ds(b * tokens, tokens), :], y_sem.at[b]) for b in range(2)]
    for copy in y_copies:
        copy.start()
    head_copy(0, 0).start()
    head_copy(0, 1).start()

    barrier = pltpu.get_barrier_semaphore()
    pl.semaphore_signal(barrier, inc=1, device_id={"ep": pair}, device_id_type=MESH)
    pl.semaphore_wait(barrier, 1)

    for copy in y_copies:
        copy.wait()

    def normalize(i):
        rows = pl.ds(pl.multiple_of(i * 16, 16), 16)
        normed[rows, :] = rms_norm(y_in[rows, :], gain_ref[...]).astype(jnp.bfloat16)

    loop(2 * tokens // 16, normalize)

    query_pos = lax.broadcasted_iota(jnp.int32, (tokens, tokens), 0)
    key_pos = lax.broadcasted_iota(jnp.int32, (tokens, tokens), 1)
    visible = (query_pos >= key_pos) & (query_pos // seq_len == key_pos // seq_len)
    score_scale = 1.0 / math.sqrt(head_dim)

    def attend(g, block, dst):
        rows = pl.ds(pl.multiple_of(block * tokens, tokens), tokens)
        for h in range(group):
            cols = slice(h * head_dim, (h + 1) * head_dim)
            scores = lax.dot_general(
                heads_qkv[0, rows, cols], heads_qkv[1, rows, cols], (((1,), (1,)), ((), ())),
                preferred_element_type=jnp.float32) * score_scale
            scores = jnp.where(visible, scores, -1e30)
            probs = jnp.exp(scores - jnp.max(scores, axis=-1, keepdims=True))
            prob_sum = jnp.sum(probs, axis=-1, keepdims=True)
            head_out = jnp.dot(
                probs.astype(jnp.bfloat16), heads_qkv[2, rows, cols], preferred_element_type=jnp.float32) / prob_sum
            dst[:, g * width + h * head_dim:g * width + (h + 1) * head_dim] = head_out.astype(jnp.bfloat16)

    for g in range(groups):
        for i in range(3):
            head_copy(g, i).wait()
            if i == 0:
                head_copy(g, 2).start()
            elif g + 1 < groups:
                head_copy(g + 1, i - 1).start()
            else:
                col_start(i - 1, i - 1)
            flat = w_heads[i].reshape(dim, width)
            heads_qkv[i] = jnp.dot(normed[...], flat, preferred_element_type=jnp.float32).astype(jnp.bfloat16)
        attend(g, 1 - core, mixed_out)
        mixed_copy(g).start()
        attend(g, core, mixed_own)

    for g in range(groups):
        mixed_copy(g).wait_recv()

    def project(n):
        slot = n % 2
        for copy in col_copies(n, slot):
            copy.wait()

        @pl.when(n >= 2)
        def _():
            out_copy(n - 2, slot).wait()
        proj = jnp.dot(mixed_own[...], w_cols[slot, 0:half], preferred_element_type=jnp.float32)
        proj = proj + jnp.dot(mixed_in[...], w_cols[slot, half:2 * half], preferred_element_type=jnp.float32)
        proj = proj.astype(jnp.bfloat16).astype(jnp.float32)
        cols = pl.ds(pl.multiple_of(n * tile, tile), tile)
        rows = pl.ds(pl.multiple_of(core * tokens, tokens), tokens)
        out_tile[slot] = (y_in[rows, cols].astype(jnp.float32) + proj).astype(jnp.bfloat16)
        out_copy(n, slot).start()

        @pl.when(n + 2 < tiles)
        def _():
            col_start(n + 2, slot)

    loop(tiles, project)
    for n in range(tiles - 2, tiles):
        out_copy(n, n % 2).wait()
    for g in range(groups):
        mixed_copy(g).wait_send()


def attention_stage(seq_len, incoming, norm_attn, w_query, w_key, w_value, w_out):
    _, tokens, dim = incoming.shape
    heads, head_dim = w_query.shape[1:]
    group = 8
    tile = 1024
    half = heads * head_dim // 2
    bf16 = jnp.bfloat16
    dma = pltpu.SemaphoreType.DMA
    vmem = pl.BlockSpec(memory_space=pltpu.VMEM)
    hbm = pl.BlockSpec(memory_space=pl.ANY)
    return pl.pallas_call(
        functools.partial(attention_kernel, seq_len),
        out_shape=jax.ShapeDtypeStruct((tokens, dim), bf16),
        in_specs=[hbm, vmem, hbm, hbm, hbm, hbm],
        out_specs=hbm,
        scratch_shapes=[
            pltpu.VMEM((2 * tokens, dim), bf16), pltpu.VMEM((2 * tokens, dim), bf16),
            pltpu.VMEM((3, dim, group, head_dim), bf16), pltpu.VMEM((2, heads * head_dim, tile), bf16),
            pltpu.VMEM((3, 2 * tokens, group * head_dim), bf16),
            pltpu.VMEM((tokens, half), bf16), pltpu.VMEM((tokens, half), bf16), pltpu.VMEM((tokens, half), bf16),
            pltpu.VMEM((2, tokens, tile), bf16),
            dma((2,)), dma((3,)), dma((2, 2)), dma((2,)), dma((heads // group // 2,)), dma((heads // group // 2,)),
        ],
        compiler_params=pltpu.CompilerParams(
            collective_id=1, has_side_effects=True, vmem_limit_bytes=67_000_000),
        name="attention_stage",
    )(incoming, norm_attn, w_query, w_key, w_value, w_out.reshape(heads * head_dim, dim))


def solution(mesh):
    ep_size = mesh.shape["ep"]
    tok_spec = P("pp", "data", "ep", None, None)
    vec_spec = P("pp", None)
    mat_spec = P("pp", None, None)
    head_spec = P("pp", None, None, None)

    def device_step(expert_out, expert_ids, slot_ids, gate_weights, residual, norm_moe, w_gate, w_up, w_down, norm_attn, w_query, w_key, w_value, w_out):
        seqs, seq_len, top_k = expert_ids.shape[2:]
        tokens = seqs * seq_len
        dim = residual.shape[-1]
        cap_slots = expert_out.shape[3] // ep_size
        first_slot = lax.axis_index("ep") * cap_slots
        slot_here = slot_ids[0, 0]
        kept_mask = slot_here >= 0
        col_ids = jnp.where(kept_mask, expert_ids[0, 0] * cap_slots + slot_here - first_slot, -1)
        weights = jnp.where(kept_mask, gate_weights[0, 0], 0.0)
        meta = jnp.concatenate([col_ids.astype(jnp.float32), weights], axis=-1).reshape(tokens, 2 * top_k)
        meta = jnp.pad(meta.T, ((0, 0), (0, 256 - tokens)))
        incoming = combine_stage(
            meta, expert_out[0, 0], residual.reshape(tokens, dim), norm_moe, w_gate[0], w_up[0], w_down[0])
        result = attention_stage(seq_len, incoming, norm_attn, w_query[0], w_key[0], w_value[0], w_out[0])
        return result.reshape(1, 1, seqs, seq_len, dim)

    in_specs = (tok_spec,) * 5 + (vec_spec, mat_spec, mat_spec, mat_spec, vec_spec, head_spec, head_spec, head_spec, head_spec)
    return jax.shard_map(device_step, mesh=mesh, in_specs=in_specs, out_specs=tok_spec, check_vma=False)
```

```python
import math
import functools
import jax
import jax.numpy as jnp
from jax import lax
from jax.experimental import pallas as pl
from jax.experimental.pallas import tpu as pltpu
from jax.sharding import PartitionSpec as P

EPSILON = 1e-6
MESH = pl.DeviceIdType.MESH
CHUNK = 32
PART = 16
COLS = 512
WIDE = 2048


def rms_norm(tensor, gain):
    values = tensor.astype(jnp.float32)
    inv_rms = lax.rsqrt(jnp.mean(values * values, axis=-1, keepdims=True) + EPSILON)
    return values * inv_rms * gain


def combine_kernel(
    meta_ref, expert_ref, resid_hbm, norm_ref, next_norm_ref, gate_hbm, up_hbm, down_hbm, x_ref, y_ref,
    tab, meta_in, meta_t, pieces, diag_out, diag_in, cross, part_out, part_in, arrive, base,
    resid, normed, hidden, y_out, y_in, w_gate, w_up, w_down,
    tab_sem, meta_send, meta_recv, diag_send, diag_recv, part_send, part_recv,
    cross_send, cross_recv, y_send, y_recv, pair_send, pair_recv, keep_sem, keep_y_sem, resid_sem, gate_sem, up_sem, down_sem,
):
    tokens, dim = resid.shape
    chunks = tokens // CHUNK
    parts = tokens // PART
    rows_owner = tab.shape[1] * tab.shape[2]
    slots = tab.shape[2]
    ff_dim = hidden.shape[1]
    me = lax.axis_index("ep")
    stage = lax.axis_index("pp")
    y_pos, core = me // 2, me % 2
    pair = y_pos * 2 + (1 - core)
    across = (1 - y_pos) * 2 + core
    diagonal = (1 - y_pos) * 2 + (1 - core)
    next_stage, prev_stage = (stage + 1) % 4, (stage + 3) % 4

    owners = (diagonal, across, pair, me)

    def table_copy(k):
        start = pl.multiple_of(owners[k] * slots, slots)
        return pltpu.make_async_copy(expert_ref.at[:, pl.ds(start, slots), :], tab.at[k], tab_sem.at[k])

    def resid_copy():
        return pltpu.make_async_copy(resid_hbm, resid, resid_sem)

    ff_tile = w_gate.shape[2]

    def gate_copy(n, slot):
        cols = pl.ds(pl.multiple_of(n * ff_tile, ff_tile), ff_tile)
        return pltpu.make_async_copy(gate_hbm.at[:, cols], w_gate.at[slot], gate_sem.at[slot])

    def up_copy(n, slot):
        cols = pl.ds(pl.multiple_of(n * ff_tile, ff_tile), ff_tile)
        return pltpu.make_async_copy(up_hbm.at[:, cols], w_up.at[slot], up_sem.at[slot])

    def down_copy(n, slot):
        cols = pl.ds(pl.multiple_of(n * COLS, COLS), COLS)
        return pltpu.make_async_copy(down_hbm.at[:, cols], w_down.at[slot], down_sem.at[slot])

    table_copy(0).start()
    table_copy(1).start()

    barrier = pltpu.get_barrier_semaphore()
    for peer in (pair, across, diagonal):
        pl.semaphore_signal(barrier, inc=1, device_id={"ep": peer}, device_id_type=MESH)
    for peer in (next_stage, prev_stage):
        pl.semaphore_signal(barrier, inc=1, device_id={"pp": peer}, device_id_type=MESH)
    pl.semaphore_wait(barrier, 5)

    def meta_copy(k):
        return pltpu.make_async_remote_copy(
            src_ref=meta_ref, dst_ref=meta_in.at[k], send_sem=meta_send.at[k], recv_sem=meta_recv.at[k],
            device_id={"ep": owners[k]}, device_id_type=MESH)

    for k in range(3):
        meta_copy(k).start()

    def rows_of(c):
        return pl.ds(pl.multiple_of(c * CHUNK, CHUNK), CHUNK)

    def row_copy(src, dst, send, recv, target, c):
        return pltpu.make_async_remote_copy(
            src_ref=src.at[rows_of(c), :], dst_ref=dst.at[rows_of(c), :], send_sem=send.at[c], recv_sem=recv.at[c],
            device_id=target, device_id_type=MESH)

    def diag_copy(c):
        return row_copy(diag_out, diag_in, diag_send, diag_recv, {"ep": pair}, c)

    def part_copy(c):
        return row_copy(part_out, part_in, part_send, part_recv, {"ep": pair}, c)

    def rows_of_part(c):
        return pl.ds(pl.multiple_of(c * PART, PART), PART)

    def part_row_copy(src, dst, send, recv, target, c):
        return pltpu.make_async_remote_copy(
            src_ref=src.at[rows_of_part(c), :], dst_ref=dst.at[rows_of_part(c), :],
            send_sem=send.at[c], recv_sem=recv.at[c], device_id=target, device_id_type=MESH)

    def cross_copy(c):
        return part_row_copy(cross, arrive, cross_send, cross_recv, {"ep": across}, c)

    def y_copy(c):
        return part_row_copy(y_out, y_in, y_send, y_recv, {"pp": next_stage}, c)

    def pair_copy(c):
        return part_row_copy(normed, x_ref.at[core], pair_send, pair_recv, {"ep": pair}, c)

    def keep_copy(c):
        rows = rows_of_part(c)
        return pltpu.make_async_copy(normed.at[rows, :], x_ref.at[core, rows, :], keep_sem.at[c])

    def keep_y_copy(c):
        rows = rows_of_part(c)
        return pltpu.make_async_copy(y_in.at[rows, :], y_ref.at[rows, :], keep_y_sem.at[c])

    def combine(k, c, dst):
        info = meta_t[k, rows_of(c), :]
        col_ids = lax.broadcasted_iota(jnp.int32, (CHUNK, rows_owner), 1) + me * rows_owner
        col_ids = col_ids.astype(jnp.float32)
        weights = jnp.zeros((CHUNK, rows_owner), jnp.float32)
        for j in range(8):
            weights = weights + jnp.where(info[:, j:j + 1] == col_ids, info[:, 8 + j:9 + j], 0.0)
        high = weights.astype(jnp.bfloat16)
        rest = weights - high.astype(jnp.float32)
        middle = rest.astype(jnp.bfloat16)
        rest = rest - middle.astype(jnp.float32)
        pieces[0:CHUNK, :] = high
        pieces[CHUNK:2 * CHUNK, :] = middle
        pieces[2 * CHUNK:3 * CHUNK, :] = rest.astype(jnp.bfloat16)

        def one_tile(n, _):
            cols = pl.ds(pl.multiple_of(n * WIDE, WIDE), WIDE)
            rows = tab[k, :, :, cols].reshape(rows_owner, WIDE)
            prod = jnp.dot(pieces[...], rows, preferred_element_type=jnp.float32)
            dst[rows_of(c), cols] = prod[0:CHUNK] + prod[CHUNK:2 * CHUNK] + prod[2 * CHUNK:3 * CHUNK]
            return 0

        lax.fori_loop(0, dim // WIDE, one_tile, 0)

    def loop(count, body):
        def step(i, _):
            body(i)
            return 0
        lax.fori_loop(0, count, step, 0)

    seqs = meta_ref.shape[0]
    seq_len = tokens // seqs

    def keep_meta(k, src):
        for q in range(seqs):
            meta_t[k, q * seq_len:(q + 1) * seq_len, :] = jnp.transpose(src[q])[0:seq_len]

    keep_meta(3, meta_ref)
    for k in range(3):
        meta_copy(k).wait_recv()
        keep_meta(k, meta_in.at[k])
    table_copy(0).wait()
    table_copy(2).start()
    table_copy(1).wait()
    table_copy(3).start()
    resid_copy().start()
    for slot in range(2):
        gate_copy(slot, slot).start()
        up_copy(slot, slot).start()
        down_copy(slot, slot).start()

    def send_diag(c):
        combine(0, c, diag_out)
        diag_copy(c).start()

    send_diag(0)

    def send_cross(c):
        combine(1, c, cross)

        @pl.when(c + 1 < chunks)
        def _():
            send_diag(c + 1)
        diag_copy(c).wait_recv()
        cross[rows_of(c), :] = cross[rows_of(c), :] + diag_in[rows_of(c), :]
        for i in range(CHUNK // PART):
            cross_copy(c * (CHUNK // PART) + i).start()

    loop(chunks, send_cross)
    table_copy(2).wait()

    def send_part(c):
        combine(2, c, part_out)
        part_copy(c).start()

    loop(chunks, send_part)
    table_copy(3).wait()
    loop(chunks, lambda c: combine(3, c, base))

    resid_copy().wait()

    def normalize(i):
        rows = pl.ds(pl.multiple_of(i * 16, 16), 16)
        normed[rows, :] = rms_norm(resid[rows, :], norm_ref[...]).astype(jnp.bfloat16)

    loop(tokens // 16, normalize)

    ff_tiles = ff_dim // ff_tile

    def gated(n):
        slot = n % 2
        gate_copy(n, slot).wait()
        up_copy(n, slot).wait()
        gate_act = jnp.dot(normed[...], w_gate[slot], preferred_element_type=jnp.float32)
        up_act = jnp.dot(normed[...], w_up[slot], preferred_element_type=jnp.float32)
        cols = pl.ds(pl.multiple_of(n * ff_tile, ff_tile), ff_tile)
        hidden[:, cols] = (jax.nn.silu(gate_act) * up_act).astype(jnp.bfloat16)

        @pl.when(n + 2 < ff_tiles)
        def _():
            gate_copy(n + 2, slot).start()
            up_copy(n + 2, slot).start()

    loop(ff_tiles, gated)
    loop(chunks, lambda c: part_copy(c).wait_recv())

    def project(n):
        slot = n % 2
        down_copy(n, slot).wait()
        shared = jnp.dot(hidden[...], w_down[slot], preferred_element_type=jnp.float32).astype(jnp.bfloat16)
        cols = pl.ds(pl.multiple_of(n * COLS, COLS), COLS)
        known = resid[:, cols].astype(jnp.float32) + shared.astype(jnp.float32)
        base[:, cols] = known + base[:, cols] + part_in[:, cols]

        @pl.when(n + 2 < dim // COLS)
        def _():
            down_copy(n + 2, slot).start()

    loop(dim // COLS, project)

    def finish(c):
        rows = rows_of_part(c)
        cross_copy(c).wait_recv()
        y_out[rows, :] = (base[rows, :] + arrive[rows, :]).astype(jnp.bfloat16)
        y_copy(c).start()

    def spread(c):
        rows = rows_of_part(c)
        y_copy(c).wait_recv()
        keep_y_copy(c).start()
        normed[rows, :] = rms_norm(y_in[rows, :], next_norm_ref[...]).astype(jnp.bfloat16)
        pair_copy(c).start()
        keep_copy(c).start()

    def finish_and_spread(c):
        finish(c + 1)
        spread(c)

    finish(0)
    loop(parts - 1, finish_and_spread)
    spread(parts - 1)

    for k in range(3):
        meta_copy(k).wait_send()

    def drain(c):
        diag_copy(c).wait_send()
        part_copy(c).wait_send()

    loop(chunks, drain)

    def drain_parts(c):
        cross_copy(c).wait_send()
        y_copy(c).wait_send()
        pair_copy(c).wait_send()
        pair_copy(c).wait_recv()
        keep_copy(c).wait()
        keep_y_copy(c).wait()

    loop(parts, drain_parts)


def combine_stage(meta, expert_out, resid, norm_moe, norm_next, w_gate, w_up, w_down):
    tokens, dim = resid.shape
    experts, slots_total, _ = expert_out.shape
    slots = slots_total // 4
    rows_owner = experts * slots
    ff_dim = w_gate.shape[1]
    chunks = tokens // CHUNK
    parts = tokens // PART
    ff_tile = 256
    f32, bf16 = jnp.float32, jnp.bfloat16
    dma = pltpu.SemaphoreType.DMA
    vmem = pl.BlockSpec(memory_space=pltpu.VMEM)
    hbm = pl.BlockSpec(memory_space=pl.ANY)
    full = (tokens, dim)
    return pl.pallas_call(
        combine_kernel,
        out_shape=(jax.ShapeDtypeStruct((2,) + full, bf16), jax.ShapeDtypeStruct(full, bf16)),
        in_specs=[vmem, hbm, hbm, vmem, vmem, hbm, hbm, hbm],
        out_specs=(hbm, hbm),
        scratch_shapes=[
            pltpu.VMEM((4, experts, slots, dim), bf16),
            pltpu.VMEM((3,) + meta.shape, f32),
            pltpu.VMEM((4, tokens, meta.shape[1]), f32),
            pltpu.VMEM((3 * CHUNK, rows_owner), bf16),
            pltpu.VMEM(full, f32), pltpu.VMEM(full, f32), pltpu.VMEM(full, f32),
            pltpu.VMEM(full, f32), pltpu.VMEM(full, f32), pltpu.VMEM(full, f32), pltpu.VMEM(full, f32),
            pltpu.VMEM(full, bf16), pltpu.VMEM(full, bf16), pltpu.VMEM((tokens, ff_dim), bf16),
            pltpu.VMEM(full, bf16), pltpu.VMEM(full, bf16),
            pltpu.VMEM((2, dim, ff_tile), bf16), pltpu.VMEM((2, dim, ff_tile), bf16),
            pltpu.VMEM((2, ff_dim, COLS), bf16),
            dma((4,)), dma((3,)), dma((3,)),
            dma((chunks,)), dma((chunks,)), dma((chunks,)), dma((chunks,)),
            dma((parts,)), dma((parts,)), dma((parts,)), dma((parts,)),
            dma((parts,)), dma((parts,)), dma((parts,)), dma((parts,)),
            dma(()), dma((2,)), dma((2,)), dma((2,)),
        ],
        compiler_params=pltpu.CompilerParams(
            collective_id=0, has_side_effects=True, vmem_limit_bytes=62 * 1024 * 1024),
        name="combine_stage",
    )(meta, expert_out, resid, norm_moe, norm_next, w_gate, w_up, w_down)


def attention_kernel(
    seq_len, x_hbm, y_hbm, query_hbm, key_hbm, value_hbm, out_w_hbm, out_hbm,
    y_in, normed, w_heads, w_cols, heads_qkv, mixed_own, mixed_out, mixed_in, out_tile,
    x_sem, y_sem, head_sem, col_sem, out_sem, mixed_send, mixed_recv,
):
    tokens, dim = y_hbm.shape
    group, head_dim = w_heads.shape[2:]
    width = group * head_dim
    groups = mixed_own.shape[1] // width
    half = groups * width
    tile = w_cols.shape[2]
    tiles = dim // tile
    weights = (query_hbm, key_hbm, value_hbm)
    me = lax.axis_index("ep")
    core = me % 2
    pair = (me // 2) * 2 + (1 - core)

    def head_copy(g, i):
        heads = pl.ds(pl.multiple_of((core * groups + g) * group, group), group)
        return pltpu.make_async_copy(weights[i].at[:, heads, :], w_heads.at[i], head_sem.at[i])

    def col_copies(n, slot):
        cols = pl.ds(pl.multiple_of(n * tile, tile), tile)
        own = pl.ds(pl.multiple_of(core * half, half), half)
        other = pl.ds(pl.multiple_of((1 - core) * half, half), half)
        return (
            pltpu.make_async_copy(out_w_hbm.at[own, cols], w_cols.at[slot, 0:half], col_sem.at[slot, 0]),
            pltpu.make_async_copy(out_w_hbm.at[other, cols], w_cols.at[slot, half:2 * half], col_sem.at[slot, 1]))

    def col_start(n, slot):
        for copy in col_copies(n, slot):
            copy.start()

    def out_copy(n, slot):
        cols = pl.ds(pl.multiple_of(n * tile, tile), tile)
        return pltpu.make_async_copy(out_tile.at[slot], out_hbm.at[:, cols], out_sem.at[slot])

    def mixed_copy(g):
        cols = pl.ds(g * width, width)
        return pltpu.make_async_remote_copy(
            src_ref=mixed_out.at[:, cols], dst_ref=mixed_in.at[:, cols], send_sem=mixed_send.at[g],
            recv_sem=mixed_recv.at[g], device_id={"ep": pair}, device_id_type=MESH)

    def loop(count, body):
        def step(i, _):
            body(i)
            return 0
        lax.fori_loop(0, count, step, 0)

    x_copies = [
        pltpu.make_async_copy(x_hbm.at[b], normed.at[pl.ds(b * tokens, tokens), :], x_sem.at[b]) for b in range(2)]
    y_copy = pltpu.make_async_copy(y_hbm, y_in, y_sem)
    for copy in x_copies:
        copy.start()
    head_copy(0, 0).start()
    head_copy(0, 1).start()
    y_copy.start()

    barrier = pltpu.get_barrier_semaphore()
    pl.semaphore_signal(barrier, inc=1, device_id={"ep": pair}, device_id_type=MESH)
    pl.semaphore_wait(barrier, 1)

    for copy in x_copies:
        copy.wait()
    y_copy.wait()

    query_pos = lax.broadcasted_iota(jnp.int32, (tokens, tokens), 0)
    key_pos = lax.broadcasted_iota(jnp.int32, (tokens, tokens), 1)
    visible = (query_pos >= key_pos) & (query_pos // seq_len == key_pos // seq_len)
    score_scale = 1.0 / math.sqrt(head_dim)

    def attend(g, block, dst):
        rows = pl.ds(pl.multiple_of(block * tokens, tokens), tokens)
        for h in range(group):
            cols = slice(h * head_dim, (h + 1) * head_dim)
            scores = lax.dot_general(
                heads_qkv[0, rows, cols], heads_qkv[1, rows, cols], (((1,), (1,)), ((), ())),
                preferred_element_type=jnp.float32) * score_scale
            scores = jnp.where(visible, scores, -1e30)
            probs = jnp.exp(scores - jnp.max(scores, axis=-1, keepdims=True))
            prob_sum = jnp.sum(probs, axis=-1, keepdims=True)
            head_out = jnp.dot(
                probs.astype(jnp.bfloat16), heads_qkv[2, rows, cols], preferred_element_type=jnp.float32) / prob_sum
            dst[:, g * width + h * head_dim:g * width + (h + 1) * head_dim] = head_out.astype(jnp.bfloat16)

    for g in range(groups):
        for i in range(3):
            head_copy(g, i).wait()
            if i == 0:
                head_copy(g, 2).start()
            elif g + 1 < groups:
                head_copy(g + 1, i - 1).start()
            else:
                col_start(i - 1, i - 1)
            flat = w_heads[i].reshape(dim, width)
            heads_qkv[i] = jnp.dot(normed[...], flat, preferred_element_type=jnp.float32).astype(jnp.bfloat16)
        attend(g, 1 - core, mixed_out)
        mixed_copy(g).start()
        attend(g, core, mixed_own)

    for g in range(groups):
        mixed_copy(g).wait_recv()

    def project(n):
        slot = n % 2
        for copy in col_copies(n, slot):
            copy.wait()

        @pl.when(n >= 2)
        def _():
            out_copy(n - 2, slot).wait()
        proj = jnp.dot(mixed_own[...], w_cols[slot, 0:half], preferred_element_type=jnp.float32)
        proj = proj + jnp.dot(mixed_in[...], w_cols[slot, half:2 * half], preferred_element_type=jnp.float32)
        proj = proj.astype(jnp.bfloat16).astype(jnp.float32)
        cols = pl.ds(pl.multiple_of(n * tile, tile), tile)
        out_tile[slot] = (y_in[:, cols].astype(jnp.float32) + proj).astype(jnp.bfloat16)
        out_copy(n, slot).start()

        @pl.when(n + 2 < tiles)
        def _():
            col_start(n + 2, slot)

    loop(tiles, project)
    for n in range(tiles - 2, tiles):
        out_copy(n, n % 2).wait()
    for g in range(groups):
        mixed_copy(g).wait_send()


def attention_stage(seq_len, normed, incoming, w_query, w_key, w_value, w_out):
    tokens, dim = incoming.shape
    heads, head_dim = w_query.shape[1:]
    group = 8
    tile = 1024
    half = heads * head_dim // 2
    bf16 = jnp.bfloat16
    dma = pltpu.SemaphoreType.DMA
    hbm = pl.BlockSpec(memory_space=pl.ANY)
    return pl.pallas_call(
        functools.partial(attention_kernel, seq_len),
        out_shape=jax.ShapeDtypeStruct((tokens, dim), bf16),
        in_specs=[hbm] * 6,
        out_specs=hbm,
        scratch_shapes=[
            pltpu.VMEM((tokens, dim), bf16), pltpu.VMEM((2 * tokens, dim), bf16),
            pltpu.VMEM((3, dim, group, head_dim), bf16), pltpu.VMEM((2, heads * head_dim, tile), bf16),
            pltpu.VMEM((3, 2 * tokens, group * head_dim), bf16),
            pltpu.VMEM((tokens, half), bf16), pltpu.VMEM((tokens, half), bf16), pltpu.VMEM((tokens, half), bf16),
            pltpu.VMEM((2, tokens, tile), bf16),
            dma((2,)), dma(()), dma((3,)), dma((2, 2)), dma((2,)), dma((heads // group // 2,)), dma((heads // group // 2,)),
        ],
        compiler_params=pltpu.CompilerParams(
            collective_id=1, has_side_effects=True, vmem_limit_bytes=67_000_000),
        name="attention_stage",
    )(normed, incoming, w_query, w_key, w_value, w_out.reshape(heads * head_dim, dim))


def solution(mesh):
    ep_size = mesh.shape["ep"]
    tok_spec = P("pp", "data", "ep", None, None)
    vec_spec = P("pp", None)
    mat_spec = P("pp", None, None)
    head_spec = P("pp", None, None, None)

    def device_step(expert_out, expert_ids, slot_ids, gate_weights, residual, norm_moe, w_gate, w_up, w_down, norm_attn, w_query, w_key, w_value, w_out):
        seqs, seq_len, top_k = expert_ids.shape[2:]
        tokens = seqs * seq_len
        dim = residual.shape[-1]
        cap_slots = expert_out.shape[3] // ep_size
        first_slot = lax.axis_index("ep") * cap_slots

        def choices_first(array):
            return jnp.swapaxes(array[0, 0], 1, 2)

        slot_here = choices_first(slot_ids)
        kept_mask = slot_here >= 0
        col_ids = jnp.where(kept_mask, choices_first(expert_ids) * cap_slots + slot_here - first_slot, -1)
        weights = jnp.where(kept_mask, choices_first(gate_weights), 0.0)
        meta = jnp.concatenate([col_ids.astype(jnp.float32), weights], axis=1)
        meta = jnp.pad(meta, ((0, 0), (0, 0), (0, 128 - seq_len)))
        normed, incoming = combine_stage(
            meta, expert_out[0, 0], residual.reshape(tokens, dim), norm_moe, norm_attn, w_gate[0], w_up[0], w_down[0])
        result = attention_stage(seq_len, normed, incoming, w_query[0], w_key[0], w_value[0], w_out[0])
        return result.reshape(1, 1, seqs, seq_len, dim)

    in_specs = (tok_spec,) * 5 + (vec_spec, mat_spec, mat_spec, mat_spec, vec_spec, head_spec, head_spec, head_spec, head_spec)
    return jax.shard_map(device_step, mesh=mesh, in_specs=in_specs, out_specs=tok_spec, check_vma=False)
```

```python
import math
import functools
import jax
import jax.numpy as jnp
from jax import lax
from jax.experimental import pallas as pl
from jax.experimental.pallas import tpu as pltpu
from jax.sharding import PartitionSpec as P

EPSILON = 1e-6
MESH = pl.DeviceIdType.MESH
CHUNK = 32
PART = 16
COLS = 512
WIDE = 2048


def rms_norm(tensor, gain):
    values = tensor.astype(jnp.float32)
    inv_rms = lax.rsqrt(jnp.mean(values * values, axis=-1, keepdims=True) + EPSILON)
    return values * inv_rms * gain


def combine_kernel(
    ids_ref, slot_ref, gates_ref, expert_ref, resid_hbm, norm_ref, next_norm_ref, gate_hbm, up_hbm, down_hbm, x_ref, y_ref,
    tab, meta_ref, meta_in, meta_t, pieces, diag_out, diag_in, cross, part_out, part_in, arrive, base,
    resid, normed, hidden, y_out, y_in, w_gate, w_up, w_down,
    tab_sem, meta_send, meta_recv, diag_send, diag_recv, part_send, part_recv,
    cross_send, cross_recv, y_send, y_recv, pair_send, pair_recv, keep_sem, keep_y_sem, resid_sem, gate_sem, up_sem, down_sem,
):
    tokens, dim = resid.shape
    chunks = tokens // CHUNK
    parts = tokens // PART
    rows_owner = tab.shape[1] * tab.shape[2]
    slots = tab.shape[2]
    ff_dim = hidden.shape[1]
    me = lax.axis_index("ep")
    stage = lax.axis_index("pp")
    y_pos, core = me // 2, me % 2
    pair = y_pos * 2 + (1 - core)
    across = (1 - y_pos) * 2 + core
    diagonal = (1 - y_pos) * 2 + (1 - core)
    next_stage, prev_stage = (stage + 1) % 4, (stage + 3) % 4

    owners = (diagonal, across, pair, me)

    def table_copy(k):
        start = pl.multiple_of(owners[k] * slots, slots)
        return pltpu.make_async_copy(expert_ref.at[:, pl.ds(start, slots), :], tab.at[k], tab_sem.at[k])

    def resid_copy():
        return pltpu.make_async_copy(resid_hbm, resid, resid_sem)

    ff_tile = w_gate.shape[2]

    def gate_copy(n, slot):
        cols = pl.ds(pl.multiple_of(n * ff_tile, ff_tile), ff_tile)
        return pltpu.make_async_copy(gate_hbm.at[:, cols], w_gate.at[slot], gate_sem.at[slot])

    def up_copy(n, slot):
        cols = pl.ds(pl.multiple_of(n * ff_tile, ff_tile), ff_tile)
        return pltpu.make_async_copy(up_hbm.at[:, cols], w_up.at[slot], up_sem.at[slot])

    def down_copy(n, slot):
        cols = pl.ds(pl.multiple_of(n * COLS, COLS), COLS)
        return pltpu.make_async_copy(down_hbm.at[:, cols], w_down.at[slot], down_sem.at[slot])

    table_copy(0).start()
    table_copy(1).start()

    seqs, choices, seq_len = ids_ref.shape
    kept = slot_ref[...] >= 0
    col_ids_own = jnp.where(kept, ids_ref[...] * slots + slot_ref[...] - me * slots, -1)
    meta_ref[...] = jnp.zeros_like(meta_ref)
    meta_ref[:, 0:choices, 0:seq_len] = col_ids_own.astype(jnp.float32)
    meta_ref[:, choices:2 * choices, 0:seq_len] = jnp.where(kept, gates_ref[...], 0.0)

    barrier = pltpu.get_barrier_semaphore()
    for peer in (pair, across, diagonal):
        pl.semaphore_signal(barrier, inc=1, device_id={"ep": peer}, device_id_type=MESH)
    for peer in (next_stage, prev_stage):
        pl.semaphore_signal(barrier, inc=1, device_id={"pp": peer}, device_id_type=MESH)
    pl.semaphore_wait(barrier, 5)

    def meta_copy(k):
        return pltpu.make_async_remote_copy(
            src_ref=meta_ref, dst_ref=meta_in.at[k], send_sem=meta_send.at[k], recv_sem=meta_recv.at[k],
            device_id={"ep": owners[k]}, device_id_type=MESH)

    for k in range(3):
        meta_copy(k).start()

    def rows_of(c):
        return pl.ds(pl.multiple_of(c * CHUNK, CHUNK), CHUNK)

    def row_copy(src, dst, send, recv, target, c):
        return pltpu.make_async_remote_copy(
            src_ref=src.at[rows_of(c), :], dst_ref=dst.at[rows_of(c), :], send_sem=send.at[c], recv_sem=recv.at[c],
            device_id=target, device_id_type=MESH)

    def diag_copy(c):
        return row_copy(diag_out, diag_in, diag_send, diag_recv, {"ep": pair}, c)

    def part_copy(c):
        return row_copy(part_out, part_in, part_send, part_recv, {"ep": pair}, c)

    def rows_of_part(c):
        return pl.ds(pl.multiple_of(c * PART, PART), PART)

    def part_row_copy(src, dst, send, recv, target, c):
        return pltpu.make_async_remote_copy(
            src_ref=src.at[rows_of_part(c), :], dst_ref=dst.at[rows_of_part(c), :],
            send_sem=send.at[c], recv_sem=recv.at[c], device_id=target, device_id_type=MESH)

    def cross_copy(c):
        return part_row_copy(cross, arrive, cross_send, cross_recv, {"ep": across}, c)

    def y_copy(c):
        return part_row_copy(y_out, y_in, y_send, y_recv, {"pp": next_stage}, c)

    def pair_copy(c):
        return part_row_copy(normed, x_ref.at[core], pair_send, pair_recv, {"ep": pair}, c)

    def keep_copy(c):
        rows = rows_of_part(c)
        return pltpu.make_async_copy(normed.at[rows, :], x_ref.at[core, rows, :], keep_sem.at[c])

    def keep_y_copy(c):
        rows = rows_of_part(c)
        return pltpu.make_async_copy(y_in.at[rows, :], y_ref.at[rows, :], keep_y_sem.at[c])

    def combine(k, c, dst):
        info = meta_t[k, rows_of(c), :]
        col_ids = lax.broadcasted_iota(jnp.int32, (CHUNK, rows_owner), 1) + me * rows_owner
        col_ids = col_ids.astype(jnp.float32)
        weights = jnp.zeros((CHUNK, rows_owner), jnp.float32)
        for j in range(8):
            weights = weights + jnp.where(info[:, j:j + 1] == col_ids, info[:, 8 + j:9 + j], 0.0)
        high = weights.astype(jnp.bfloat16)
        rest = weights - high.astype(jnp.float32)
        middle = rest.astype(jnp.bfloat16)
        rest = rest - middle.astype(jnp.float32)
        pieces[0:CHUNK, :] = high
        pieces[CHUNK:2 * CHUNK, :] = middle
        pieces[2 * CHUNK:3 * CHUNK, :] = rest.astype(jnp.bfloat16)

        def one_tile(n, _):
            cols = pl.ds(pl.multiple_of(n * WIDE, WIDE), WIDE)
            rows = tab[k, :, :, cols].reshape(rows_owner, WIDE)
            prod = jnp.dot(pieces[...], rows, preferred_element_type=jnp.float32)
            dst[rows_of(c), cols] = prod[0:CHUNK] + prod[CHUNK:2 * CHUNK] + prod[2 * CHUNK:3 * CHUNK]
            return 0

        lax.fori_loop(0, dim // WIDE, one_tile, 0)

    def loop(count, body):
        def step(i, _):
            body(i)
            return 0
        lax.fori_loop(0, count, step, 0)

    def keep_meta(k, src):
        for q in range(seqs):
            meta_t[k, q * seq_len:(q + 1) * seq_len, :] = jnp.transpose(src[q])[0:seq_len]

    keep_meta(3, meta_ref)
    for k in range(3):
        meta_copy(k).wait_recv()
        keep_meta(k, meta_in.at[k])
    table_copy(0).wait()
    table_copy(2).start()
    table_copy(1).wait()
    table_copy(3).start()
    resid_copy().start()
    for slot in range(2):
        gate_copy(slot, slot).start()
        up_copy(slot, slot).start()
        down_copy(slot, slot).start()

    def send_diag(c):
        combine(0, c, diag_out)
        diag_copy(c).start()

    send_diag(0)

    def send_cross(c):
        combine(1, c, cross)

        @pl.when(c + 1 < chunks)
        def _():
            send_diag(c + 1)
        diag_copy(c).wait_recv()
        cross[rows_of(c), :] = cross[rows_of(c), :] + diag_in[rows_of(c), :]
        for i in range(CHUNK // PART):
            cross_copy(c * (CHUNK // PART) + i).start()

    loop(chunks, send_cross)
    table_copy(2).wait()

    def send_part(c):
        combine(2, c, part_out)
        part_copy(c).start()

    loop(chunks, send_part)
    table_copy(3).wait()
    loop(chunks, lambda c: combine(3, c, base))

    resid_copy().wait()

    def normalize(i):
        rows = pl.ds(pl.multiple_of(i * 16, 16), 16)
        normed[rows, :] = rms_norm(resid[rows, :], norm_ref[...]).astype(jnp.bfloat16)

    loop(tokens // 16, normalize)

    ff_tiles = ff_dim // ff_tile

    def gated(n):
        slot = n % 2
        gate_copy(n, slot).wait()
        up_copy(n, slot).wait()
        gate_act = jnp.dot(normed[...], w_gate[slot], preferred_element_type=jnp.float32)
        up_act = jnp.dot(normed[...], w_up[slot], preferred_element_type=jnp.float32)
        cols = pl.ds(pl.multiple_of(n * ff_tile, ff_tile), ff_tile)
        hidden[:, cols] = (jax.nn.silu(gate_act) * up_act).astype(jnp.bfloat16)

        @pl.when(n + 2 < ff_tiles)
        def _():
            gate_copy(n + 2, slot).start()
            up_copy(n + 2, slot).start()

    loop(ff_tiles, gated)
    loop(chunks, lambda c: part_copy(c).wait_recv())

    def project(n):
        slot = n % 2
        down_copy(n, slot).wait()
        shared = jnp.dot(hidden[...], w_down[slot], preferred_element_type=jnp.float32).astype(jnp.bfloat16)
        cols = pl.ds(pl.multiple_of(n * COLS, COLS), COLS)
        known = resid[:, cols].astype(jnp.float32) + shared.astype(jnp.float32)
        base[:, cols] = known + base[:, cols] + part_in[:, cols]

        @pl.when(n + 2 < dim // COLS)
        def _():
            down_copy(n + 2, slot).start()

    loop(dim // COLS, project)

    def finish(c):
        rows = rows_of_part(c)
        cross_copy(c).wait_recv()
        y_out[rows, :] = (base[rows, :] + arrive[rows, :]).astype(jnp.bfloat16)
        y_copy(c).start()

    def spread(c):
        rows = rows_of_part(c)
        y_copy(c).wait_recv()
        keep_y_copy(c).start()
        normed[rows, :] = rms_norm(y_in[rows, :], next_norm_ref[...]).astype(jnp.bfloat16)
        pair_copy(c).start()
        keep_copy(c).start()

    def finish_and_spread(c):
        finish(c + 1)
        spread(c)

    finish(0)
    loop(parts - 1, finish_and_spread)
    spread(parts - 1)

    for k in range(3):
        meta_copy(k).wait_send()

    def drain(c):
        diag_copy(c).wait_send()
        part_copy(c).wait_send()

    loop(chunks, drain)

    def drain_parts(c):
        cross_copy(c).wait_send()
        y_copy(c).wait_send()
        pair_copy(c).wait_send()
        pair_copy(c).wait_recv()
        keep_copy(c).wait()
        keep_y_copy(c).wait()

    loop(parts, drain_parts)


def combine_stage(ids, slot_ids, gates, expert_out, resid, norm_moe, norm_next, w_gate, w_up, w_down):
    tokens, dim = resid.shape
    experts, slots_total, _ = expert_out.shape
    slots = slots_total // 4
    rows_owner = experts * slots
    ff_dim = w_gate.shape[1]
    chunks = tokens // CHUNK
    parts = tokens // PART
    ff_tile = 256
    f32, bf16 = jnp.float32, jnp.bfloat16
    dma = pltpu.SemaphoreType.DMA
    vmem = pl.BlockSpec(memory_space=pltpu.VMEM)
    hbm = pl.BlockSpec(memory_space=pl.ANY)
    full = (tokens, dim)
    meta_shape = (ids.shape[0], 2 * ids.shape[1], 128)
    return pl.pallas_call(
        combine_kernel,
        out_shape=(jax.ShapeDtypeStruct((2,) + full, bf16), jax.ShapeDtypeStruct(full, bf16)),
        in_specs=[vmem, vmem, vmem, hbm, hbm, vmem, vmem, hbm, hbm, hbm],
        out_specs=(hbm, hbm),
        scratch_shapes=[
            pltpu.VMEM((4, experts, slots, dim), bf16),
            pltpu.VMEM(meta_shape, f32),
            pltpu.VMEM((3,) + meta_shape, f32),
            pltpu.VMEM((4, tokens, meta_shape[1]), f32),
            pltpu.VMEM((3 * CHUNK, rows_owner), bf16),
            pltpu.VMEM(full, f32), pltpu.VMEM(full, f32), pltpu.VMEM(full, f32),
            pltpu.VMEM(full, f32), pltpu.VMEM(full, f32), pltpu.VMEM(full, f32), pltpu.VMEM(full, f32),
            pltpu.VMEM(full, bf16), pltpu.VMEM(full, bf16), pltpu.VMEM((tokens, ff_dim), bf16),
            pltpu.VMEM(full, bf16), pltpu.VMEM(full, bf16),
            pltpu.VMEM((2, dim, ff_tile), bf16), pltpu.VMEM((2, dim, ff_tile), bf16),
            pltpu.VMEM((2, ff_dim, COLS), bf16),
            dma((4,)), dma((3,)), dma((3,)),
            dma((chunks,)), dma((chunks,)), dma((chunks,)), dma((chunks,)),
            dma((parts,)), dma((parts,)), dma((parts,)), dma((parts,)),
            dma((parts,)), dma((parts,)), dma((parts,)), dma((parts,)),
            dma(()), dma((2,)), dma((2,)), dma((2,)),
        ],
        compiler_params=pltpu.CompilerParams(
            collective_id=0, has_side_effects=True, vmem_limit_bytes=62 * 1024 * 1024),
        name="combine_stage",
    )(ids, slot_ids, gates, expert_out, resid, norm_moe, norm_next, w_gate, w_up, w_down)


def attention_kernel(
    seq_len, x_hbm, query_hbm, key_hbm, value_hbm, out_w_hbm, out_hbm,
    normed, w_heads, w_cols, heads_qkv, mixed_own, mixed_out, mixed_in, out_tile,
    x_sem, head_sem, col_sem, out_sem, mixed_send, mixed_recv,
):
    _, tokens, dim = x_hbm.shape
    group, head_dim = w_heads.shape[2:]
    width = group * head_dim
    groups = mixed_own.shape[1] // width
    half = groups * width
    tile = w_cols.shape[2]
    tiles = dim // tile
    weights = (query_hbm, key_hbm, value_hbm)
    me = lax.axis_index("ep")
    core = me % 2
    pair = (me // 2) * 2 + (1 - core)

    def head_copy(g, i):
        heads = pl.ds(pl.multiple_of((core * groups + g) * group, group), group)
        return pltpu.make_async_copy(weights[i].at[:, heads, :], w_heads.at[i], head_sem.at[i])

    def col_copies(n, slot):
        cols = pl.ds(pl.multiple_of(n * tile, tile), tile)
        own = pl.ds(pl.multiple_of(core * half, half), half)
        other = pl.ds(pl.multiple_of((1 - core) * half, half), half)
        return (
            pltpu.make_async_copy(out_w_hbm.at[own, cols], w_cols.at[slot, 0:half], col_sem.at[slot, 0]),
            pltpu.make_async_copy(out_w_hbm.at[other, cols], w_cols.at[slot, half:2 * half], col_sem.at[slot, 1]))

    def col_start(n, slot):
        for copy in col_copies(n, slot):
            copy.start()

    def out_copy(n, slot):
        cols = pl.ds(pl.multiple_of(n * tile, tile), tile)
        return pltpu.make_async_copy(out_tile.at[slot], out_hbm.at[:, cols], out_sem.at[slot])

    def mixed_copy(g):
        cols = pl.ds(g * width, width)
        return pltpu.make_async_remote_copy(
            src_ref=mixed_out.at[:, cols], dst_ref=mixed_in.at[:, cols], send_sem=mixed_send.at[g],
            recv_sem=mixed_recv.at[g], device_id={"ep": pair}, device_id_type=MESH)

    def loop(count, body):
        def step(i, _):
            body(i)
            return 0
        lax.fori_loop(0, count, step, 0)

    x_copies = [
        pltpu.make_async_copy(x_hbm.at[b], normed.at[pl.ds(b * tokens, tokens), :], x_sem.at[b]) for b in range(2)]
    for copy in x_copies:
        copy.start()
    head_copy(0, 0).start()

    barrier = pltpu.get_barrier_semaphore()
    pl.semaphore_signal(barrier, inc=1, device_id={"ep": pair}, device_id_type=MESH)
    pl.semaphore_wait(barrier, 1)

    for copy in x_copies:
        copy.wait()

    query_pos = lax.broadcasted_iota(jnp.int32, (tokens, tokens), 0)
    key_pos = lax.broadcasted_iota(jnp.int32, (tokens, tokens), 1)
    visible = (query_pos >= key_pos) & (query_pos // seq_len == key_pos // seq_len)
    score_scale = 1.0 / math.sqrt(head_dim)

    def attend(g, block, dst):
        rows = pl.ds(pl.multiple_of(block * tokens, tokens), tokens)
        for h in range(group):
            cols = slice(h * head_dim, (h + 1) * head_dim)
            scores = lax.dot_general(
                heads_qkv[0, rows, cols], heads_qkv[1, rows, cols], (((1,), (1,)), ((), ())),
                preferred_element_type=jnp.float32) * score_scale
            scores = jnp.where(visible, scores, -1e30)
            probs = jnp.exp(scores - jnp.max(scores, axis=-1, keepdims=True))
            prob_sum = jnp.sum(probs, axis=-1, keepdims=True)
            head_out = jnp.dot(
                probs.astype(jnp.bfloat16), heads_qkv[2, rows, cols], preferred_element_type=jnp.float32) / prob_sum
            dst[:, g * width + h * head_dim:g * width + (h + 1) * head_dim] = head_out.astype(jnp.bfloat16)

    for g in range(groups):
        for i in range(3):
            head_copy(g, i).wait()
            if i < 2:
                head_copy(g, i + 1).start()
            elif g + 1 < groups:
                head_copy(g + 1, 0).start()
            else:
                col_start(0, 0)
                col_start(1, 1)
            flat = w_heads[i].reshape(dim, width)
            heads_qkv[i] = jnp.dot(normed[...], flat, preferred_element_type=jnp.float32).astype(jnp.bfloat16)
        attend(g, 1 - core, mixed_out)
        mixed_copy(g).start()
        attend(g, core, mixed_own)

    for g in range(groups):
        mixed_copy(g).wait_recv()

    def project(n):
        slot = n % 2
        for copy in col_copies(n, slot):
            copy.wait()

        @pl.when(n >= 2)
        def _():
            out_copy(n - 2, slot).wait()
        proj = jnp.dot(mixed_own[...], w_cols[slot, 0:half], preferred_element_type=jnp.float32)
        proj = proj + jnp.dot(mixed_in[...], w_cols[slot, half:2 * half], preferred_element_type=jnp.float32)
        out_tile[slot] = proj.astype(jnp.bfloat16)
        out_copy(n, slot).start()

        @pl.when(n + 2 < tiles)
        def _():
            col_start(n + 2, slot)

    loop(tiles, project)
    for n in range(tiles - 2, tiles):
        out_copy(n, n % 2).wait()
    for g in range(groups):
        mixed_copy(g).wait_send()


def attention_stage(seq_len, normed, w_query, w_key, w_value, w_out):
    _, tokens, dim = normed.shape
    heads, head_dim = w_query.shape[1:]
    group = 8
    tile = 1024
    half = heads * head_dim // 2
    bf16 = jnp.bfloat16
    dma = pltpu.SemaphoreType.DMA
    hbm = pl.BlockSpec(memory_space=pl.ANY)
    return pl.pallas_call(
        functools.partial(attention_kernel, seq_len),
        out_shape=jax.ShapeDtypeStruct((tokens, dim), bf16),
        in_specs=[hbm] * 5,
        out_specs=hbm,
        scratch_shapes=[
            pltpu.VMEM((2 * tokens, dim), bf16),
            pltpu.VMEM((3, dim, group, head_dim), bf16), pltpu.VMEM((2, heads * head_dim, tile), bf16),
            pltpu.VMEM((3, 2 * tokens, group * head_dim), bf16),
            pltpu.VMEM((tokens, half), bf16), pltpu.VMEM((tokens, half), bf16), pltpu.VMEM((tokens, half), bf16),
            pltpu.VMEM((2, tokens, tile), bf16),
            dma((2,)), dma((3,)), dma((2, 2)), dma((2,)), dma((heads // group // 2,)), dma((heads // group // 2,)),
        ],
        compiler_params=pltpu.CompilerParams(
            collective_id=1, has_side_effects=True, vmem_limit_bytes=67_000_000),
        name="attention_stage",
    )(normed, w_query, w_key, w_value, w_out.reshape(heads * head_dim, dim))


def solution(mesh):
    tok_spec = P("pp", "data", "ep", None, None)
    vec_spec = P("pp", None)
    mat_spec = P("pp", None, None)
    head_spec = P("pp", None, None, None)

    def device_step(expert_out, expert_ids, slot_ids, gate_weights, residual, norm_moe, w_gate, w_up, w_down, norm_attn, w_query, w_key, w_value, w_out):
        seqs, seq_len = expert_ids.shape[2:4]
        tokens = seqs * seq_len
        dim = residual.shape[-1]

        def choices_first(array):
            return jnp.swapaxes(array[0, 0], 1, 2)

        normed, incoming = combine_stage(
            choices_first(expert_ids), choices_first(slot_ids), choices_first(gate_weights), expert_out[0, 0],
            residual.reshape(tokens, dim), norm_moe, norm_attn, w_gate[0], w_up[0], w_down[0])
        projected = attention_stage(seq_len, normed, w_query[0], w_key[0], w_value[0], w_out[0])
        result = (incoming.astype(jnp.float32) + projected.astype(jnp.float32)).astype(jnp.bfloat16)
        return result.reshape(1, 1, seqs, seq_len, dim)

    in_specs = (tok_spec,) * 5 + (vec_spec, mat_spec, mat_spec, mat_spec, vec_spec, head_spec, head_spec, head_spec, head_spec)
    return jax.shard_map(device_step, mesh=mesh, in_specs=in_specs, out_specs=tok_spec, check_vma=False)
```
